32 devices in a mesh: band: 16 (over z, y, core), ga: 2 (over x).
Axes of the slice: x: 2, y: 2, z: 4, core: 2. Of those that a mesh axis runs over, the one named last changes fastest.
Arguments:
- orbitals: bfloat16 [2, 16, 160, 128], P(None, 'band', 'ga'), may hold values from -8 to 8, as said below
- potential: float32 [480, 480], P('ga'), may hold values from -2 to 2
- slot_sticks: int32 [160], replicated, may hold values from -1 to 126, as said below
- stick_entries: int32 [160, 128], replicated, may hold values from -1 to 126, as said below
Outputs:
- applied_orbitals: bfloat16 [2, 16, 160, 128], P(None, 'band', 'ga')
- correlation: float32 [2, 16, 16], replicated
- reduced_hamiltonian: float32 [2, 16, 16], replicated
The draws below stay inside these ranges and needn't reach their ends.
Inputs may be any that keep to these rules, and one draw needn't show every extreme that they name: `slot_sticks`: every gx with |gx| < 64 is held by exactly one slot; the other slots hold -1. Slots t with t // 80 = d are those of index d of ga; on some index of ga all 80 slots hold sticks. `stick_entries`: row t lists, in some order, gz + 63 for every gz with gx^2 + gz^2 < 64^2, gx being the stick of slot t, then -1 to the end of the row; rows of empty slots are all -1. `orbitals`: entries where stick_entries is -1 carry values that are not used.
All inputs are finite; a program needn't handle non-finite values.
Results may differ from the reference program's by a relative error of at most 0.001.
Values may be sent and summed in bfloat16 or wider, within the bound.
No kernel may reach another device: no remote copies, remote signals or barrier semaphores. Data moves between devices by JAX's collectives and lax.ppermute only.
A program may use at most 64 MiB of HBM per device.

```python
import jax
import jax.numpy as jnp
from jax import lax

NGRID = 480
RAD = 64
KMAX = 128
SLOTS = 80
SLOT_ALL = 160
NB = 16
N_GA = 2


def stick_layout(key):
    stick_count = 2 * RAD - 1
    key_device, key_picked, key_ordering = jax.random.split(jax.random.fold_in(key, 11), 3)
    full_device = jax.random.randint(key_device, (), 0, N_GA)
    slot_ids = jnp.arange(SLOT_ALL, dtype=jnp.int32)
    owners = slot_ids // SLOTS
    others = jnp.where(owners > full_device, slot_ids - SLOTS, slot_ids)
    picked = jax.random.permutation(key_picked, (N_GA - 1) * SLOTS).astype(jnp.int32)
    chosen = jnp.take(picked, jnp.clip(others, 0, (N_GA - 1) * SLOTS - 1)) < stick_count - SLOTS
    occupied = jnp.where(owners == full_device, True, chosen)
    ranking = jnp.cumsum(occupied.astype(jnp.int32)) - 1
    ordering = jax.random.permutation(key_ordering, stick_count).astype(jnp.int32)
    return jnp.where(occupied, jnp.take(ordering, jnp.clip(ranking, 0, stick_count - 1)), -1).astype(jnp.int32)


def draw_slot_sticks(key, part):
    return stick_layout(key)


def draw_stick_entries(key, part):
    sticks = stick_layout(key)
    gx_value = sticks - RAD + 1
    offsets = jnp.arange(RAD, dtype=jnp.int32)
    half_width = jnp.sum((offsets * offsets)[None, :] + (gx_value * gx_value)[:, None] < RAD * RAD, axis=1).astype(jnp.int32) - 1
    length = jnp.where(sticks >= 0, 2 * half_width + 1, 0)
    column_ids = jnp.arange(KMAX, dtype=jnp.int32)
    inside = column_ids[None, :] < length[:, None]
    positions = jnp.where(inside, RAD - 1 - half_width[:, None] + column_ids[None, :], -1)
    jitter = jax.random.randint(jax.random.fold_in(key, 23), (SLOT_ALL, KMAX), 0, 4096)
    scores = jnp.where(inside, jitter, 4096) * KMAX + column_ids[None, :]
    ordering = jnp.argsort(scores, axis=1)
    return jnp.take_along_axis(positions, ordering, axis=1).astype(jnp.int32)


def draw_orbitals(key, part):
    key_own, key_common, key_weight, key_flip = jax.random.split(jax.random.fold_in(key, 37), 4)
    private = jax.random.normal(key_own, (2, NB, SLOT_ALL, KMAX), jnp.float32)
    weight = jax.random.uniform(key_weight, (NB,), jnp.float32, 0.5, 1.5)
    common = jax.random.normal(key_common, (2, 1, SLOT_ALL, KMAX), jnp.float32)
    sign_flip = jnp.where(jax.random.bernoulli(key_flip, 0.5, (NB,)), 1.0, -1.0)
    values = private + (weight * sign_flip)[None, :, None, None] * common
    return jnp.clip(values, -8.0, 8.0).astype(jnp.bfloat16)


def steps_of(rng, shape, pieces, smallest, high):
    loudness, own = 1.0, jax.random.fold_in(rng, 6)
    for dim, parts in pieces:
        steps = jnp.exp(jax.random.uniform(jax.random.fold_in(own, dim), (parts,), jnp.float32, smallest / len(pieces), high / len(pieces)))
        loudness = loudness * jnp.repeat(steps, shape[dim] // parts).reshape([-1 if axis == dim else 1 for axis in range(len(shape))])
    return loudness


def setup_inputs(seed: int = 0) -> dict:
    key_of = jax.random.split(jax.random.key(seed), 5)
    return {
        "orbitals": draw_orbitals(jax.random.fold_in(key_of[4], 71), 0),
        "potential": jnp.clip(jax.random.uniform(key_of[1], (NGRID, NGRID), jnp.float32, -2.0, 2.0) * steps_of(key_of[1], (NGRID, NGRID), ((0, 2),), -0.4, 0.0), -2.0, 2.0),
        "slot_sticks": draw_slot_sticks(jax.random.fold_in(key_of[4], 71), 0),
        "stick_entries": draw_stick_entries(jax.random.fold_in(key_of[4], 71), 0),
    }


TWO_PI = 6.283185307179586
HIGHEST_PRECISION = lax.Precision.HIGHEST


def phases(frequency, position, points):
    winding = (frequency[:, None] * position[None, :]) % points
    angles = winding.astype(jnp.float32) * (TWO_PI / points)
    return jnp.cos(angles), jnp.sin(angles)


def stick_phases(slot_sticks, radius, points):
    frequency = slot_sticks - radius + 1
    x_cos, x_sin = phases(frequency, jnp.arange(points, dtype=jnp.int32), points)
    filled = (slot_sticks >= 0).astype(jnp.float32)[:, None]
    return x_cos * filled, x_sin * filled


def unpack(coeffs, entry_lists):
    slot_count, width = entry_lists.shape
    leading = coeffs.shape[:2]
    flat_index = jnp.where(entry_lists >= 0, entry_lists + width * jnp.arange(slot_count, dtype=jnp.int32)[:, None], slot_count * width)
    spread = jnp.zeros(leading + (slot_count * width,), jnp.float32)
    values = coeffs.reshape(leading + (slot_count * width,)).astype(jnp.float32)
    spread = spread.at[:, :, flat_index.reshape(-1)].add(values, mode="drop")
    return spread.reshape(coeffs.shape)


def z_forward(spread, z_cos, z_sin):
    real_part = jnp.einsum("bsp,pz->bsz", spread[0], z_cos, precision=HIGHEST_PRECISION) - jnp.einsum("bsp,pz->bsz", spread[1], z_sin, precision=HIGHEST_PRECISION)
    imag_part = jnp.einsum("bsp,pz->bsz", spread[0], z_sin, precision=HIGHEST_PRECISION) + jnp.einsum("bsp,pz->bsz", spread[1], z_cos, precision=HIGHEST_PRECISION)
    return jnp.stack([real_part, imag_part])


def plane_work(columns, x_cos, x_sin, potential):
    field_real = jnp.einsum("bsz,sx->bzx", columns[0], x_cos, precision=HIGHEST_PRECISION) - jnp.einsum("bsz,sx->bzx", columns[1], x_sin, precision=HIGHEST_PRECISION)
    field_imag = jnp.einsum("bsz,sx->bzx", columns[0], x_sin, precision=HIGHEST_PRECISION) + jnp.einsum("bsz,sx->bzx", columns[1], x_cos, precision=HIGHEST_PRECISION)
    prod_real = potential[None] * field_real
    prod_imag = potential[None] * field_imag
    back_real = jnp.einsum("bzx,sx->bsz", prod_real, x_cos, precision=HIGHEST_PRECISION) + jnp.einsum("bzx,sx->bsz", prod_imag, x_sin, precision=HIGHEST_PRECISION)
    back_imag = jnp.einsum("bzx,sx->bsz", prod_imag, x_cos, precision=HIGHEST_PRECISION) - jnp.einsum("bzx,sx->bsz", prod_real, x_sin, precision=HIGHEST_PRECISION)
    return jnp.stack([back_real, back_imag])


def z_backward(gathered, z_cos, z_sin, points):
    real_part = jnp.einsum("bsz,pz->bsp", gathered[0], z_cos, precision=HIGHEST_PRECISION) + jnp.einsum("bsz,pz->bsp", gathered[1], z_sin, precision=HIGHEST_PRECISION)
    imag_part = jnp.einsum("bsz,pz->bsp", gathered[1], z_cos, precision=HIGHEST_PRECISION) - jnp.einsum("bsz,pz->bsp", gathered[0], z_sin, precision=HIGHEST_PRECISION)
    return jnp.stack([real_part, imag_part]) / float(points * points)


def kinetic_factor(sticks, entry_lists, radius):
    gx_value = sticks - radius + 1
    gz_value = entry_lists - radius + 1
    return ((gx_value * gx_value)[:, None] + gz_value * gz_value).astype(jnp.float32) / float(radius * radius)


def cross_products(left, right, scale):
    dims = (((1,), (1,)), ((), ()))
    real_part = lax.dot_general(left[0], right[0], dims, preferred_element_type=jnp.float32) + lax.dot_general(left[1], right[1], dims, preferred_element_type=jnp.float32)
    imag_part = lax.dot_general(left[0], right[1], dims, preferred_element_type=jnp.float32) - lax.dot_general(left[1], right[0], dims, preferred_element_type=jnp.float32)
    return jnp.stack([real_part, imag_part]) * scale


def reference(orbitals, potential, slot_sticks, stick_entries):
    points = potential.shape[1]
    width = stick_entries.shape[1]
    radius = width // 2
    band_total = orbitals.shape[1]
    present = stick_entries >= 0
    masked = jnp.where(present[None, None], orbitals, jnp.zeros_like(orbitals))
    spread = unpack(orbitals, stick_entries)
    frequency = jnp.arange(width, dtype=jnp.int32) - radius + 1
    z_cos, z_sin = phases(frequency, jnp.arange(points, dtype=jnp.int32), points)
    x_cos, x_sin = stick_phases(slot_sticks, radius, points)

    def one_band(coeffs):
        columns = z_forward(coeffs[:, None], z_cos, z_sin)
        gathered = plane_work(columns, x_cos, x_sin, potential)
        return z_backward(gathered, z_cos, z_sin, points)[:, 0]

    spectra = jnp.moveaxis(lax.map(one_band, jnp.moveaxis(spread, 1, 0)), 0, 1)
    indices = jnp.broadcast_to(jnp.clip(stick_entries, 0, width - 1)[None, None], spectra.shape)
    applied = jnp.take_along_axis(spectra, indices, axis=3)
    kinetic = kinetic_factor(slot_sticks, stick_entries, radius)
    applied_orbitals = jnp.where(present[None, None], kinetic[None, None] * orbitals.astype(jnp.float32) + applied, jnp.float32(0.0)).astype(jnp.bfloat16)
    scale = 1.0 / (4.0 * radius * radius)
    flat_psi = masked.reshape(2, band_total, -1)
    flat_h = applied_orbitals.reshape(2, band_total, -1)
    correlation = cross_products(flat_psi, flat_psi, scale)
    reduced_hamiltonian = cross_products(flat_psi, flat_h, scale)
    return applied_orbitals, correlation, reduced_hamiltonian
```

```python
import math

import jax
import jax.numpy as jnp
import numpy as np
from jax import lax
from jax.experimental import pallas as pl
from jax.experimental.pallas import tpu as pltpu
from jax.sharding import PartitionSpec as P

F32 = jnp.float32
BF16 = jnp.bfloat16
VMEM_SPEC = pl.BlockSpec(memory_space=pltpu.VMEM)
SMEM_SPEC = pl.BlockSpec(memory_space=pltpu.SMEM)


def hi_lo_table(values):
    high = jnp.asarray(values, F32).astype(BF16)
    high_np = np.asarray(values, np.float32).astype(jnp.bfloat16)
    low_np = (values - high_np.astype(np.float64)).astype(jnp.bfloat16)
    return high_np, low_np


def twiddle_tables(points, radius, group_count):
    width = 2 * radius
    planes = points // group_count
    z = np.arange(points, dtype=np.int64)
    gz = np.arange(width, dtype=np.int64) - radius + 1
    angle_z = (z[:, None] * gz[None, :] % points) * (2.0 * np.pi / points)
    forward = np.concatenate([np.cos(angle_z), np.sin(angle_z)], axis=1)
    forward = forward.reshape(group_count, planes, 2 * width)
    backward = np.ascontiguousarray(np.transpose(forward, (0, 2, 1)))
    gx = np.arange(radius, dtype=np.int64)
    angle_x = (gx[:, None] * z[None, :] % points) * (2.0 * np.pi / points)
    x_table = np.concatenate([np.cos(angle_x), np.sin(angle_x)], axis=0)
    z_high, z_low = hi_lo_table(forward)
    zt_high, zt_low = hi_lo_table(backward)
    x_high, x_low = hi_lo_table(x_table)
    xt = np.concatenate([x_high.T, x_low.T], axis=1)
    return z_high, z_low, zt_high, zt_low, x_high, x_low, xt


def split(values):
    high = values.astype(BF16)
    low = (values - high.astype(F32)).astype(BF16)
    return high, low


def dot(left, right):
    return jnp.dot(left, right, preferred_element_type=F32)


def canonical_lane(sticks, radius):
    gx = sticks - radius + 1
    return jnp.where(gx >= 0, gx, radius - gx)


def spread_kernel(ga_ref, orbitals_ref, entries_ref, sticks_ref, out_ref, e_ref, re_ref, im_ref):
    width = entries_ref.shape[2]
    radius = width // 2
    slots = entries_ref.shape[1]
    ga = ga_ref[0]
    e_ref[...] = entries_ref[ga].astype(F32).T
    re_ref[...] = orbitals_ref[0, 0].astype(F32).T
    im_ref[...] = orbitals_ref[1, 0].astype(F32).T
    position = lax.broadcasted_iota(jnp.int32, (width, slots), 0).astype(F32)

    def step(k, carry):
        real_part, imag_part = carry
        match = e_ref[pl.ds(k, 1), :] == position
        real_part = jnp.where(match, re_ref[pl.ds(k, 1), :], real_part)
        imag_part = jnp.where(match, im_ref[pl.ds(k, 1), :], imag_part)
        return real_part, imag_part

    zeros = jnp.zeros((width, slots), F32)
    real_part, imag_part = lax.fori_loop(0, width, step, (zeros, zeros), unroll=4)
    spread = jnp.concatenate([real_part, imag_part], axis=0).astype(BF16)
    lane = canonical_lane(sticks_ref[ga], radius)
    choose = (lax.broadcasted_iota(jnp.int32, (width, slots), 0) == lane).astype(F32).astype(BF16)
    out_ref[...] = lax.dot_general(
        spread, choose, (((1,), (1,)), ((), ())), preferred_element_type=F32
    ).astype(BF16)


def grid_kernel(ga_ref, coeffs_refs, potential_ref, sticks_ref, tables, own_ref, send_ref):
    z_high, z_low, zt_high, zt_low, x_high, x_low, xt = tables
    planes, points = potential_ref.shape
    width = coeffs_refs[0].shape[1]
    radius = width // 2
    groups, _, slots = sticks_ref.shape
    ga = ga_ref[0]
    coeffs = coeffs_refs[0][...].astype(F32)
    for ref in coeffs_refs[1:]:
        coeffs = coeffs + ref[...].astype(F32)
    real_part, imag_part = coeffs[:width], coeffs[width:]
    rows = jnp.concatenate(
        [
            jnp.concatenate([real_part, imag_part], axis=1),
            jnp.concatenate([-imag_part, real_part], axis=1),
        ],
        axis=0,
    ).astype(BF16)
    columns = dot(z_high[ga], rows) + dot(z_low[ga], rows)
    col_re, col_im = columns[:, :width], columns[:, width:]
    rol_re, rol_im = pltpu.roll(col_re, radius, 1), pltpu.roll(col_im, radius, 1)
    even = lax.broadcasted_iota(jnp.int32, (planes, width), 1) < radius
    parity = jnp.concatenate(
        [
            jnp.where(even, col_re + rol_re, col_im - rol_im),
            jnp.where(even, col_im + rol_im, rol_re - col_re),
        ],
        axis=0,
    )
    par_high, par_low = split(parity)
    table = x_high[...]
    field = dot(jnp.concatenate([par_high, par_low], axis=1), jnp.concatenate([table, table], axis=0))
    field = field + dot(par_high, x_low[...])
    values = potential_ref[...]
    product = jnp.concatenate([values, values], axis=0) * field
    prod_high, prod_low = split(product)
    table_t = xt[...]
    wide = dot(prod_high, table_t)
    back = wide[:, :width] + wide[:, width:] + dot(prod_low, table_t[:, :width])
    back_re, back_im = back[:planes], back[planes:]
    rol_re, rol_im = pltpu.roll(back_re, radius, 1), pltpu.roll(back_im, radius, 1)
    gathered = jnp.concatenate(
        [
            jnp.where(even, back_re + rol_im, rol_re - back_im),
            jnp.where(even, back_im - rol_re, rol_im + back_re),
        ],
        axis=1,
    )
    gat_high, gat_low = split(gathered)
    spectra = dot(zt_high[ga], gat_high) + dot(zt_low[ga], gat_high) + dot(zt_high[ga], gat_low)
    spectra = jnp.concatenate(
        [
            spectra[:width, :width] + spectra[width:, width:],
            spectra[:width, width:] - spectra[width:, :width],
        ],
        axis=0,
    )
    spec_high, spec_low = split(spectra)
    spec = jnp.concatenate([spec_high, spec_low], axis=1)
    lanes = lax.broadcasted_iota(jnp.int32, (slots, width), 1)
    for distance in range(groups):
        lane_row = canonical_lane(sticks_ref[lax.rem(ga + distance, groups)], radius).astype(F32)
        lane_col = jnp.broadcast_to(lane_row, (width, slots)).T.astype(jnp.int32)
        choose = (lane_col == lanes).astype(F32).astype(BF16)
        picked = lax.dot_general(
            jnp.concatenate([choose, choose], axis=1), spec, (((1,), (1,)), ((), ())), preferred_element_type=F32
        )
        if distance == 0:
            own_ref[...] = picked
        else:
            send_ref[distance - 1] = picked


def apply_part(ga, partial_refs, orbitals_ref, entries_ref, sticks_ref, points):
    width = entries_ref.shape[2]
    radius = width // 2
    total = partial_refs[0][...]
    for ref in partial_refs[1:]:
        total = total + ref[...]
    entries = entries_ref[ga]
    present = entries >= 0
    index = jnp.maximum(entries, 0)
    gx_row = (sticks_ref[ga] - radius + 1).astype(F32)
    gx = jnp.broadcast_to(gx_row, (width, gx_row.shape[1])).T
    gz = (entries - radius + 1).astype(F32)
    kinetic = (gx * gx + gz * gz) * (1.0 / (radius * radius))
    result = []
    for part in range(2):
        picked = jnp.take_along_axis(
            total[:, part * width : (part + 1) * width], index, axis=1, mode="promise_in_bounds"
        )
        value = kinetic * orbitals_ref[part, 0].astype(F32) + picked * (1.0 / (points * points))
        result.append(jnp.where(present, value, 0.0).astype(BF16))
    return result, present


def final_kernel(points, ga_ref, partial_refs, orbitals_ref, entries_ref, sticks_ref, psi_refs, out_ref, sums_ref):
    ga = ga_ref[0]
    result, present = apply_part(ga, partial_refs, orbitals_ref, entries_ref, sticks_ref, points)
    for part in range(2):
        out_ref[part, 0] = result[part]
    slots, width = present.shape
    h_re, h_im = result[0].astype(F32), result[1].astype(F32)
    m_re = jnp.where(present, orbitals_ref[0, 0].astype(F32), 0.0)
    m_im = jnp.where(present, orbitals_ref[1, 0].astype(F32), 0.0)
    rows = [[], [], [], []]
    for psi_ref in psi_refs:
        for band in range(psi_ref.shape[1]):
            left_re = psi_ref[0, band].astype(F32)
            left_im = psi_ref[1, band].astype(F32)
            for place, (right_re, right_im) in enumerate(((m_re, m_im), (h_re, h_im))):
                rows[2 * place].append(jnp.sum(left_re * right_re + left_im * right_im, axis=0, keepdims=True))
                rows[2 * place + 1].append(jnp.sum(left_re * right_im - left_im * right_re, axis=0, keepdims=True))
    flat = sum(rows, [])
    lanes = sums_ref.shape[1]
    if len(flat) < lanes:
        flat.append(jnp.zeros((lanes - len(flat), width), F32))
    sums = jnp.sum(jnp.concatenate(flat, axis=0).T, axis=0, keepdims=True)
    sums_ref[...] = jnp.broadcast_to(sums, sums_ref.shape)


def assemble_kernel(groups, inner, blocks, scale, sums_ref, corr_ref, ham_ref):
    bands = inner * blocks
    shifts = blocks // 2 + 1
    count = shifts * inner
    total = sums_ref[0:bands, :]
    for group in range(1, groups):
        total = total + sums_ref[group * bands : (group + 1) * bands, :]
    lanes = total.shape[1]
    total = jnp.concatenate([total, jnp.zeros((lanes - bands, lanes), F32)], axis=0).T * scale
    row = lax.broadcasted_iota(jnp.int32, (lanes, lanes), 0)
    col = lax.broadcasted_iota(jnp.int32, (lanes, lanes), 1)
    row, col = row[:bands], col[:bands]
    shift_bits = int(math.log2(inner))
    row_block = lax.shift_right_logical(row, shift_bits)
    col_block = lax.shift_right_logical(col, shift_bits)
    away = row_block - col_block
    away = jnp.where(away < 0, away + blocks, away)
    slot = away * inner + lax.bitwise_xor(lax.bitwise_and(row, inner - 1), lax.bitwise_and(col, inner - 1))
    covered = away < shifts
    for place, ref in enumerate((corr_ref, ham_ref)):
        for part in range(2):
            base = (2 * place + part) * count
            direct = jnp.zeros((bands, lanes), F32)
            for index in range(count):
                direct = jnp.where(slot == index, total[base + index : base + index + 1, :], direct)
            padded = jnp.concatenate([direct, jnp.zeros((lanes - bands, lanes), F32)], axis=0)
            mirror = padded.T[:bands]
            if part:
                mirror = -mirror
            ref[part] = jnp.where(covered, direct, mirror)[:, :bands]


def general_matrices(psi, masked, applied, inner, blocks, scale):
    bands = inner * blocks
    shifts = blocks // 2 + 1
    count = shifts * inner
    left = jnp.concatenate(psi, axis=1).reshape(2, count, -1)
    right = jnp.stack([masked.reshape(2, -1), applied.reshape(2, -1)])
    product = jnp.einsum("cin,mdn->mcdi", left, right, preferred_element_type=F32)
    block = jnp.stack([product[:, 0, 0] + product[:, 1, 1], product[:, 0, 1] - product[:, 1, 0]], axis=1)
    everywhere = lax.all_gather(lax.psum(block * scale, "ga"), "band", axis=0)
    row, col = np.meshgrid(np.arange(bands), np.arange(bands), indexing="ij")
    away = (row // inner - col // inner) % blocks
    slot = np.where(away < shifts, away * inner + ((row % inner) ^ (col % inner)), 0)
    flat = jnp.transpose(everywhere, (1, 2, 0, 3)).reshape(4 * bands, count)
    index = jnp.asarray(np.tile(slot.T, (4, 1)), jnp.int32)
    direct = jnp.take_along_axis(flat, index, axis=1).reshape(2, 2, bands, bands)
    direct = jnp.swapaxes(direct, 2, 3)
    sign = jnp.asarray([1.0, -1.0], F32)[None, :, None, None]
    full = jnp.where(jnp.asarray(away < shifts), direct, sign * jnp.swapaxes(direct, 2, 3))
    return full[0], full[1]


def body(band_total, groups, orbitals, potential, slot_sticks, stick_entries):
    planes, points = potential.shape
    width = stick_entries.shape[1]
    radius = width // 2
    slots = orbitals.shape[2]
    inner = math.gcd(band_total, 4)
    blocks = band_total // inner
    shifts = blocks // 2 + 1
    ga = lax.axis_index("ga").astype(jnp.int32).reshape(1)
    entries = stick_entries.reshape(groups, slots, width)
    sticks = slot_sticks.reshape(groups, 1, slots)
    tables = [jnp.asarray(t) for t in twiddle_tables(points, radius, groups)]

    near = [orbitals]
    for shift in range(1, shifts):
        pairs = [(i, (i - inner * shift) % band_total) for i in range(band_total)]
        near.append(lax.ppermute(orbitals, "band", pairs))

    coeffs = pl.pallas_call(
        spread_kernel,
        out_shape=jax.ShapeDtypeStruct((2 * width, width), BF16),
        in_specs=[SMEM_SPEC, VMEM_SPEC, VMEM_SPEC, VMEM_SPEC],
        out_specs=VMEM_SPEC,
        scratch_shapes=[pltpu.VMEM((width, slots), F32)] * 3,
        name="spread",
    )(ga, orbitals, entries, sticks)
    all_coeffs = [coeffs]
    for distance in range(1, groups):
        pairs = [(i, (i + distance) % groups) for i in range(groups)]
        all_coeffs.append(lax.ppermute(coeffs, "ga", pairs))

    psi = [jnp.concatenate(near, axis=1)]
    step = inner // 2
    while step:
        pairs = [(i, i ^ step) for i in range(band_total)]
        psi = psi + [lax.ppermute(part, "band", pairs) for part in psi]
        step //= 2
    order = [0]
    step = inner // 2
    while step:
        order = order + [o ^ step for o in order]
        step //= 2
    psi = [psi[order.index(q)] for q in range(inner)]

    def run_grid(ga_ref, *refs):
        count = len(all_coeffs)
        grid_kernel(ga_ref, refs[:count], refs[count], refs[count + 1], refs[count + 2 : count + 9], *refs[count + 9 :])

    own, send = pl.pallas_call(
        run_grid,
        out_shape=(
            jax.ShapeDtypeStruct((slots, 2 * width), F32),
            jax.ShapeDtypeStruct((groups - 1, slots, 2 * width), F32),
        ),
        in_specs=[SMEM_SPEC] + [VMEM_SPEC] * (len(all_coeffs) + 9),
        out_specs=(VMEM_SPEC, VMEM_SPEC),
        name="grid",
    )(ga, *all_coeffs, potential, sticks, *tables)
    partials = [own]
    for distance in range(1, groups):
        pairs = [(i, (i + distance) % groups) for i in range(groups)]
        partials.append(lax.ppermute(send[distance - 1], "ga", pairs))

    scale = 1.0 / (4.0 * radius * radius)
    out_type = jax.ShapeDtypeStruct(orbitals.shape, BF16)
    small = 4 * shifts * inner <= 128 and band_total <= 128
    count = len(partials)
    if not small:

        def run_apply(ga_ref, *refs):
            result, _ = apply_part(ga_ref[0], refs[:count], *refs[count : count + 3], points)
            refs[count + 3][0, 0] = result[0]
            refs[count + 3][1, 0] = result[1]

        applied = pl.pallas_call(
            run_apply,
            out_shape=out_type,
            in_specs=[SMEM_SPEC] + [VMEM_SPEC] * (count + 3),
            out_specs=VMEM_SPEC,
            name="apply",
        )(ga, *partials, orbitals, entries, sticks)
        own_lists = lax.dynamic_index_in_dim(entries, ga[0], 0, keepdims=False)
        masked = jnp.where(own_lists >= 0, orbitals, jnp.zeros_like(orbitals))
        left = [p for p in psi]
        left = [jnp.stack(left, axis=2).reshape(2, shifts * inner, slots, width)]
        correlation, reduced = general_matrices(left, masked, applied, inner, blocks, scale)
        return applied, correlation, reduced

    def run_final(ga_ref, *refs):
        rest = refs[count + 3 :]
        final_kernel(
            points, ga_ref, refs[:count], *refs[count : count + 3], [SplitBands(rest[:inner], s) for s in range(shifts)], *rest[inner:]
        )

    applied, sums = pl.pallas_call(
        run_final,
        out_shape=(out_type, jax.ShapeDtypeStruct((groups * band_total, 128), F32)),
        in_specs=[SMEM_SPEC] + [VMEM_SPEC] * (count + 3 + inner),
        out_specs=(VMEM_SPEC, VMEM_SPEC),
        name="final",
    )(ga, *partials, orbitals, entries, sticks, *psi)
    everywhere = lax.all_to_all(sums, ("ga", "band"), split_axis=0, concat_axis=0, tiled=True)
    matrix = jax.ShapeDtypeStruct((2, band_total, band_total), F32)

    def run_assemble(sums_ref, corr_ref, ham_ref):
        assemble_kernel(groups, inner, blocks, scale, sums_ref, corr_ref, ham_ref)

    correlation, reduced = pl.pallas_call(
        run_assemble,
        out_shape=(matrix, matrix),
        in_specs=[VMEM_SPEC],
        out_specs=(VMEM_SPEC, VMEM_SPEC),
        name="assemble",
    )(everywhere)
    return applied, correlation, reduced


class SplitBands:
    def __init__(self, refs, shift):
        self.refs = refs
        self.shift = shift
        self.shape = (2, len(refs))

    def __getitem__(self, key):
        part, band = key
        return self.refs[band][part, self.shift]


def solution(mesh):
    band_total = mesh.shape["band"]
    groups = mesh.shape["ga"]

    def mapped(orbitals, potential, slot_sticks, stick_entries):
        return body(band_total, groups, orbitals, potential, slot_sticks, stick_entries)

    return jax.shard_map(
        mapped,
        mesh=mesh,
        in_specs=(P(None, "band", "ga", None), P("ga", None), P(), P()),
        out_specs=(P(None, "band", "ga", None), P(), P()),
        check_vma=False,
    )
```

```python
import math

import jax
import jax.numpy as jnp
import numpy as np
from jax import lax
from jax.experimental import pallas as pl
from jax.experimental.pallas import tpu as pltpu
from jax.sharding import PartitionSpec as P


F32 = jnp.float32
BF16 = jnp.bfloat16
VMEM_SPEC = pl.BlockSpec(memory_space=pltpu.VMEM)
SMEM_SPEC = pl.BlockSpec(memory_space=pltpu.SMEM)
FIRST_FLOPS = 3_000_000_000
SPREAD_FLOPS = 1_500_000_000
GRID_FLOPS = 3_000_000_000
KERNEL_PARAMS = pltpu.CompilerParams(vmem_limit_bytes=16 * 1024 * 1024)


def hi_lo_table(values):
    high = jnp.asarray(values, F32).astype(BF16)
    high_np = np.asarray(values, np.float32).astype(jnp.bfloat16)
    low_np = (values - high_np.astype(np.float64)).astype(jnp.bfloat16)
    return high_np, low_np


def twiddle_tables(points, radius, group_count):
    width = 2 * radius
    planes = points // group_count
    z = np.arange(points, dtype=np.int64)
    gz = np.arange(width, dtype=np.int64) - radius + 1
    angle_z = (z[:, None] * gz[None, :] % points) * (2.0 * np.pi / points)
    forward = np.concatenate([np.cos(angle_z), np.sin(angle_z)], axis=1)
    forward = forward.reshape(group_count, planes, 2 * width)
    backward = np.ascontiguousarray(np.transpose(forward, (0, 2, 1)))
    gx = np.arange(radius, dtype=np.int64)
    angle_x = (gx[:, None] * z[None, :] % points) * (2.0 * np.pi / points)
    x_table = np.concatenate([np.cos(angle_x), np.sin(angle_x)], axis=0)
    z_high, z_low = hi_lo_table(forward)
    zt_high, zt_low = hi_lo_table(backward)
    x_high, x_low = hi_lo_table(x_table)
    xt = np.concatenate([x_high.T, x_low.T], axis=1)
    return z_high, z_low, zt_high, zt_low, x_high, x_low, xt


def split(values):
    high = values.astype(BF16)
    low = (values - high.astype(F32)).astype(BF16)
    return high, low


def dot(left, right):
    return jnp.dot(left, right, preferred_element_type=F32)


def canonical_lane(sticks, radius):
    gx = sticks - radius + 1
    return jnp.where(gx >= 0, gx, radius - gx)


def rows_kernel(out_ref):
    out_ref[...] = lax.broadcasted_iota(jnp.int32, out_ref.shape, 0).astype(F32)


def sticks_of(sticks_ref, group, slots):
    sticks = sticks_ref[...]
    row = sticks[:, :slots]
    for index in range(1, sticks.shape[1] // slots):
        row = jnp.where(group == index, sticks[:, index * slots : (index + 1) * slots], row)
    return row


def spread_kernel(ga_ref, rows_ref, orbitals_ref, entries_ref, sticks_ref, out_ref, e_ref, re_ref, im_ref):
    width = entries_ref.shape[2]
    radius = width // 2
    slots = entries_ref.shape[1]
    ga = ga_ref[0]
    e_ref[...] = entries_ref[ga].astype(F32).T
    re_ref[...] = orbitals_ref[0, 0].astype(F32).T
    im_ref[...] = orbitals_ref[1, 0].astype(F32).T
    position = rows_ref[...]

    def step(k, carry):
        real_part, imag_part = carry
        match = e_ref[pl.ds(k, 1), :] == position
        real_part = jnp.where(match, re_ref[pl.ds(k, 1), :], real_part)
        imag_part = jnp.where(match, im_ref[pl.ds(k, 1), :], imag_part)
        return real_part, imag_part

    zeros = jnp.zeros((width, slots), F32)
    real_part, imag_part = lax.fori_loop(0, width, step, (zeros, zeros), unroll=4)
    spread = jnp.concatenate([real_part, imag_part], axis=0).astype(BF16)
    lane = canonical_lane(sticks_of(sticks_ref, ga, slots), radius)
    choose = (lax.broadcasted_iota(jnp.int32, (width, slots), 0) == lane).astype(F32).astype(BF16)
    out_ref[...] = lax.dot_general(
        spread, choose, (((1,), (1,)), ((), ())), preferred_element_type=F32
    ).astype(BF16)


def grid_kernel(ga_ref, coeffs_refs, potential_ref, sticks_ref, tables, own_ref, send_ref):
    z_high, z_low, zt_high, zt_low, x_high, x_low, xt = tables
    planes, _ = potential_ref.shape
    width = coeffs_refs[0].shape[1]
    radius = width // 2
    slots = own_ref.shape[0]
    groups = sticks_ref.shape[1] // slots
    ga = ga_ref[0]
    coeffs = coeffs_refs[0][...].astype(F32)
    for ref in coeffs_refs[1:]:
        coeffs = coeffs + ref[...].astype(F32)
    real_part, imag_part = coeffs[:width], coeffs[width:]
    rows = jnp.concatenate(
        [
            jnp.concatenate([real_part, imag_part], axis=1),
            jnp.concatenate([-imag_part, real_part], axis=1),
        ],
        axis=0,
    ).astype(BF16)
    columns = dot(z_high[ga], rows) + dot(z_low[ga], rows)
    col_re, col_im = columns[:, :width], columns[:, width:]
    rol_re, rol_im = pltpu.roll(col_re, radius, 1), pltpu.roll(col_im, radius, 1)
    even = lax.broadcasted_iota(jnp.int32, (planes, width), 1) < radius
    parity = jnp.concatenate(
        [
            jnp.where(even, col_re + rol_re, col_im - rol_im),
            jnp.where(even, col_im + rol_im, rol_re - col_re),
        ],
        axis=0,
    )
    par_high, par_low = split(parity)
    table = x_high[...]
    field = dot(jnp.concatenate([par_high, par_low], axis=1), jnp.concatenate([table, table], axis=0))
    field = field + dot(par_high, x_low[...])
    values = potential_ref[...]
    product = jnp.concatenate([values, values], axis=0) * field
    prod_high, prod_low = split(product)
    table_t = xt[...]
    wide = dot(prod_high, table_t)
    back = wide[:, :width] + wide[:, width:] + dot(prod_low, table_t[:, :width])
    back_re, back_im = back[:planes], back[planes:]
    rol_re, rol_im = pltpu.roll(back_re, radius, 1), pltpu.roll(back_im, radius, 1)
    gathered = jnp.concatenate(
        [
            jnp.where(even, back_re + rol_im, rol_re - back_im),
            jnp.where(even, back_im - rol_re, rol_im + back_re),
        ],
        axis=1,
    )
    gat_high, gat_low = split(gathered)
    spectra = dot(zt_high[ga], gat_high) + dot(zt_low[ga], gat_high) + dot(zt_high[ga], gat_low)
    spectra = jnp.concatenate(
        [
            spectra[:width, :width] + spectra[width:, width:],
            spectra[:width, width:] - spectra[width:, :width],
        ],
        axis=0,
    )
    spec_high, spec_low = split(spectra)
    spec = jnp.concatenate([spec_high, spec_low], axis=1)
    lanes = lax.broadcasted_iota(jnp.int32, (slots, width), 1)
    for distance in range(groups):
        group = lax.rem(ga + distance, groups)
        lane_row = canonical_lane(sticks_of(sticks_ref, group, slots), radius).astype(F32)
        lane_col = jnp.broadcast_to(lane_row, (width, slots)).T.astype(jnp.int32)
        choose = (lane_col == lanes).astype(F32).astype(BF16)
        picked = lax.dot_general(
            jnp.concatenate([choose, choose], axis=1), spec, (((1,), (1,)), ((), ())), preferred_element_type=F32
        )
        if distance == 0:
            own_ref[...] = picked
        else:
            send_ref[distance - 1] = picked


def apply_part(ga, partial_refs, orbitals_ref, entries_ref, sticks_ref, points):
    width = entries_ref.shape[2]
    radius = width // 2
    total = partial_refs[0][...]
    for ref in partial_refs[1:]:
        total = total + ref[...]
    entries = entries_ref[ga]
    present = entries >= 0
    index = jnp.maximum(entries, 0)
    gx_row = (sticks_of(sticks_ref, ga, entries.shape[0]) - radius + 1).astype(F32)
    gx = jnp.broadcast_to(gx_row, (width, gx_row.shape[1])).T
    gz = (entries - radius + 1).astype(F32)
    kinetic = (gx * gx + gz * gz) * (1.0 / (radius * radius))
    result = []
    for part in range(2):
        picked = jnp.take_along_axis(
            total[:, part * width : (part + 1) * width], index, axis=1, mode="promise_in_bounds"
        )
        value = kinetic * orbitals_ref[part, 0].astype(F32) + picked * (1.0 / (points * points))
        result.append(jnp.where(present, value, 0.0).astype(BF16))
    return result, present


def final_kernel(points, ga_ref, partial_refs, orbitals_ref, entries_ref, sticks_ref, psi_refs, out_ref, sums_ref):
    ga = ga_ref[0]
    result, present = apply_part(ga, partial_refs, orbitals_ref, entries_ref, sticks_ref, points)
    for part in range(2):
        out_ref[part, 0] = result[part]
    _, width = present.shape
    h_re, h_im = result[0].astype(F32), result[1].astype(F32)
    m_re = jnp.where(present, orbitals_ref[0, 0].astype(F32), 0.0)
    m_im = jnp.where(present, orbitals_ref[1, 0].astype(F32), 0.0)
    rows = [[], [], [], []]
    for psi_ref in psi_refs:
        for band in range(psi_ref.shape[1]):
            left_re = psi_ref[0, band].astype(F32)
            left_im = psi_ref[1, band].astype(F32)
            for place, (right_re, right_im) in enumerate(((m_re, m_im), (h_re, h_im))):
                rows[2 * place].append(jnp.sum(left_re * right_re + left_im * right_im, axis=0, keepdims=True))
                rows[2 * place + 1].append(jnp.sum(left_re * right_im - left_im * right_re, axis=0, keepdims=True))
    flat = sum(rows, [])
    lanes = sums_ref.shape[1]
    if len(flat) < lanes:
        flat.append(jnp.zeros((lanes - len(flat), width), F32))
    sums = jnp.sum(jnp.concatenate(flat, axis=0).T, axis=0, keepdims=True)
    sums_ref[...] = jnp.broadcast_to(sums, sums_ref.shape)


def assemble_kernel(groups, inner, blocks, scale, sums_ref, corr_ref, ham_ref):
    bands = inner * blocks
    shifts = blocks // 2 + 1
    count = shifts * inner
    total = sums_ref[0:bands, :]
    for group in range(1, groups):
        total = total + sums_ref[group * bands : (group + 1) * bands, :]
    lanes = total.shape[1]
    total = jnp.concatenate([total, jnp.zeros((lanes - bands, lanes), F32)], axis=0).T * scale
    row = lax.broadcasted_iota(jnp.int32, (lanes, lanes), 0)
    col = lax.broadcasted_iota(jnp.int32, (lanes, lanes), 1)
    row, col = row[:bands], col[:bands]
    shift_bits = int(math.log2(inner))
    row_block = lax.shift_right_logical(row, shift_bits)
    col_block = lax.shift_right_logical(col, shift_bits)
    away = row_block - col_block
    away = jnp.where(away < 0, away + blocks, away)
    slot = away * inner + lax.bitwise_xor(lax.bitwise_and(row, inner - 1), lax.bitwise_and(col, inner - 1))
    covered = away < shifts
    for place, ref in enumerate((corr_ref, ham_ref)):
        for part in range(2):
            base = (2 * place + part) * count
            direct = jnp.zeros((bands, lanes), F32)
            for index in range(count):
                direct = jnp.where(slot == index, total[base + index : base + index + 1, :], direct)
            padded = jnp.concatenate([direct, jnp.zeros((lanes - bands, lanes), F32)], axis=0)
            mirror = padded.T[:bands]
            if part:
                mirror = -mirror
            ref[part] = jnp.where(covered, direct, mirror)[:, :bands]


def general_matrices(psi, masked, applied, inner, blocks, scale):
    bands = inner * blocks
    shifts = blocks // 2 + 1
    count = shifts * inner
    left = jnp.concatenate(psi, axis=1).reshape(2, count, -1)
    right = jnp.stack([masked.reshape(2, -1), applied.reshape(2, -1)])
    product = jnp.einsum("cin,mdn->mcdi", left, right, preferred_element_type=F32)
    block = jnp.stack([product[:, 0, 0] + product[:, 1, 1], product[:, 0, 1] - product[:, 1, 0]], axis=1)
    everywhere = lax.all_gather(lax.psum(block * scale, "ga"), "band", axis=0)
    row, col = np.meshgrid(np.arange(bands), np.arange(bands), indexing="ij")
    away = (row // inner - col // inner) % blocks
    slot = np.where(away < shifts, away * inner + ((row % inner) ^ (col % inner)), 0)
    flat = jnp.transpose(everywhere, (1, 2, 0, 3)).reshape(4 * bands, count)
    index = jnp.asarray(np.tile(slot.T, (4, 1)), jnp.int32)
    direct = jnp.take_along_axis(flat, index, axis=1).reshape(2, 2, bands, bands)
    direct = jnp.swapaxes(direct, 2, 3)
    sign = jnp.asarray([1.0, -1.0], F32)[None, :, None, None]
    full = jnp.where(jnp.asarray(away < shifts), direct, sign * jnp.swapaxes(direct, 2, 3))
    return full[0], full[1]


def body(band_total, groups, orbitals, potential, slot_sticks, stick_entries):
    _, points = potential.shape
    width = stick_entries.shape[1]
    radius = width // 2
    slots = orbitals.shape[2]
    inner = math.gcd(band_total, 4)
    blocks = band_total // inner
    shifts = blocks // 2 + 1
    ga = lax.axis_index("ga").astype(jnp.int32).reshape(1)
    entries = stick_entries.reshape(groups, slots, width)
    sticks = slot_sticks.reshape(1, groups * slots)
    tables = [jnp.asarray(t) for t in twiddle_tables(points, radius, groups)]

    rows = pl.pallas_call(
        rows_kernel,
        out_shape=jax.ShapeDtypeStruct((width, slots), F32),
        out_specs=VMEM_SPEC,
        compiler_params=KERNEL_PARAMS,
        cost_estimate=pl.CostEstimate(flops=FIRST_FLOPS, bytes_accessed=0, transcendentals=0),
        name="rows",
    )()
    orbitals, rows = lax.optimization_barrier((orbitals, rows))
    near = [orbitals]
    for shift in range(1, shifts):
        pairs = [(i, (i - inner * shift) % band_total) for i in range(band_total)]
        near.append(lax.ppermute(orbitals, "band", pairs))

    place = pl.pallas_call(
        spread_kernel,
        out_shape=jax.ShapeDtypeStruct((2 * width, width), BF16),
        in_specs=[SMEM_SPEC] + [VMEM_SPEC] * 4,
        out_specs=VMEM_SPEC,
        scratch_shapes=[pltpu.VMEM((width, slots), F32)] * 3,
        compiler_params=KERNEL_PARAMS,
        cost_estimate=pl.CostEstimate(flops=SPREAD_FLOPS, bytes_accessed=0, transcendentals=0),
        name="spread",
    )
    coeffs = place(ga, rows, orbitals, entries, sticks)
    all_coeffs = [coeffs]
    for distance in range(1, groups):
        pairs = [(i, (i + distance) % groups) for i in range(groups)]
        all_coeffs.append(lax.ppermute(coeffs, "ga", pairs))

    received, *near = lax.optimization_barrier((all_coeffs[-1], *near))
    all_coeffs[-1] = received
    psi, order, step = [jnp.concatenate(near, axis=1)], [0], inner // 2

    def widen(parts, order, step):
        pairs = [(i, i ^ step) for i in range(band_total)]
        return parts + [lax.ppermute(part, "band", pairs) for part in parts], order + [o ^ step for o in order]

    while step > 1:
        psi, order = widen(psi, order, step)
        step //= 2

    def run_grid(ga_ref, *refs):
        count = len(all_coeffs)
        grid_kernel(ga_ref, refs[:count], refs[count], refs[count + 1], refs[count + 2 : count + 9], *refs[count + 9 :])

    own, send = pl.pallas_call(
        run_grid,
        out_shape=(
            jax.ShapeDtypeStruct((slots, 2 * width), F32),
            jax.ShapeDtypeStruct((groups - 1, slots, 2 * width), F32),
        ),
        in_specs=[SMEM_SPEC] + [VMEM_SPEC] * (len(all_coeffs) + 9),
        out_specs=(VMEM_SPEC, VMEM_SPEC),
        compiler_params=KERNEL_PARAMS,
        cost_estimate=pl.CostEstimate(flops=GRID_FLOPS, bytes_accessed=0, transcendentals=0),
        name="grid",
    )(ga, *all_coeffs, potential, sticks, *tables)
    own, *psi = lax.optimization_barrier((own, *psi))
    if step:
        psi, order = widen(psi, order, step)
    psi = [psi[order.index(q)] for q in range(inner)]
    partials = [own]
    for distance in range(1, groups):
        pairs = [(i, (i + distance) % groups) for i in range(groups)]
        partials.append(lax.ppermute(send[distance - 1], "ga", pairs))

    scale = 1.0 / (4.0 * radius * radius)
    out_type = jax.ShapeDtypeStruct(orbitals.shape, BF16)
    small = 4 * shifts * inner <= 128 and band_total <= 128
    count = len(partials)
    if not small:

        def run_apply(ga_ref, *refs):
            result, _ = apply_part(ga_ref[0], refs[:count], *refs[count : count + 3], points)
            refs[count + 3][0, 0] = result[0]
            refs[count + 3][1, 0] = result[1]

        applied = pl.pallas_call(
            run_apply,
            out_shape=out_type,
            in_specs=[SMEM_SPEC] + [VMEM_SPEC] * (count + 3),
            out_specs=VMEM_SPEC,
            compiler_params=KERNEL_PARAMS,
            name="apply",
        )(ga, *partials, orbitals, entries, sticks)
        own_lists = lax.dynamic_index_in_dim(entries, ga[0], 0, keepdims=False)
        masked = jnp.where(own_lists >= 0, orbitals, jnp.zeros_like(orbitals))
        left = [p for p in psi]
        left = [jnp.stack(left, axis=2).reshape(2, shifts * inner, slots, width)]
        correlation, reduced = general_matrices(left, masked, applied, inner, blocks, scale)
        return applied, correlation, reduced

    def run_final(ga_ref, *refs):
        rest = refs[count + 3 :]
        final_kernel(
            points, ga_ref, refs[:count], *refs[count : count + 3], [SplitBands(rest[:inner], s) for s in range(shifts)], *rest[inner:]
        )

    applied, sums = pl.pallas_call(
        run_final,
        out_shape=(out_type, jax.ShapeDtypeStruct((groups * band_total, 128), F32)),
        in_specs=[SMEM_SPEC] + [VMEM_SPEC] * (count + 3 + inner),
        out_specs=(VMEM_SPEC, VMEM_SPEC),
        compiler_params=KERNEL_PARAMS,
        name="final",
    )(ga, *partials, orbitals, entries, sticks, *psi)
    everywhere = lax.all_to_all(sums, ("ga", "band"), split_axis=0, concat_axis=0, tiled=True)
    matrix = jax.ShapeDtypeStruct((2, band_total, band_total), F32)

    def run_assemble(sums_ref, corr_ref, ham_ref):
        assemble_kernel(groups, inner, blocks, scale, sums_ref, corr_ref, ham_ref)

    correlation, reduced = pl.pallas_call(
        run_assemble,
        out_shape=(matrix, matrix),
        in_specs=[VMEM_SPEC],
        out_specs=(VMEM_SPEC, VMEM_SPEC),
        compiler_params=KERNEL_PARAMS,
        name="assemble",
    )(everywhere)
    return applied, correlation, reduced


class SplitBands:
    def __init__(self, refs, shift):
        self.refs = refs
        self.shift = shift
        self.shape = (2, len(refs))

    def __getitem__(self, key):
        part, band = key
        return self.refs[band][part, self.shift]


def solution(mesh):
    band_total = mesh.shape["band"]
    groups = mesh.shape["ga"]

    def mapped(orbitals, potential, slot_sticks, stick_entries):
        return body(band_total, groups, orbitals, potential, slot_sticks, stick_entries)

    return jax.shard_map(
        mapped,
        mesh=mesh,
        in_specs=(P(None, "band", "ga", None), P("ga", None), P(), P()),
        out_specs=(P(None, "band", "ga", None), P(), P()),
        check_vma=False,
    )
```

```python
import functools
import math

import jax
import jax.numpy as jnp
import numpy as np
from jax import lax
from jax.experimental import pallas as pl
from jax.experimental.pallas import tpu as pltpu
from jax.sharding import PartitionSpec as P


F32 = jnp.float32
BF16 = jnp.bfloat16
VMEM_SPEC = pl.BlockSpec(memory_space=pltpu.VMEM)
SMEM_SPEC = pl.BlockSpec(memory_space=pltpu.SMEM)
FIRST_FLOPS = 3_000_000_000
SPREAD_FLOPS = 1_500_000_000
GRID_FLOPS = 3_000_000_000
KERNEL_PARAMS = pltpu.CompilerParams(vmem_limit_bytes=16 * 1024 * 1024)


def hi_lo_table(values):
    high = jnp.asarray(values, F32).astype(BF16)
    high_np = np.asarray(values, np.float32).astype(jnp.bfloat16)
    low_np = (values - high_np.astype(np.float64)).astype(jnp.bfloat16)
    return high_np, low_np


def twiddle_tables(points, radius, group_count):
    width = 2 * radius
    planes = points // group_count
    z = np.arange(points, dtype=np.int64)
    gz = np.arange(width, dtype=np.int64) - radius + 1
    angle_z = (z[:, None] * gz[None, :] % points) * (2.0 * np.pi / points)
    forward = np.concatenate([np.cos(angle_z), np.sin(angle_z)], axis=1)
    forward = forward.reshape(group_count, planes, 2 * width)
    backward = np.ascontiguousarray(np.transpose(forward, (0, 2, 1)))
    gx = np.arange(radius, dtype=np.int64)
    angle_x = (gx[:, None] * z[None, :] % points) * (2.0 * np.pi / points)
    x_table = np.concatenate([np.cos(angle_x), np.sin(angle_x)], axis=0)
    z_high, z_low = hi_lo_table(forward)
    zt_high, zt_low = hi_lo_table(backward)
    x_high, x_low = hi_lo_table(x_table)
    xt = np.concatenate([x_high.T, x_low.T], axis=1)
    return np.stack([z_high, z_low], 1), np.stack([zt_high, zt_low], 1), np.stack([x_high, x_low]), xt


def split(values):
    high = values.astype(BF16)
    low = (values - high.astype(F32)).astype(BF16)
    return high, low


def dot(left, right):
    return jnp.dot(left, right, preferred_element_type=F32)


def dot_rows(left, right):
    return lax.dot_general(left, right, (((1,), (1,)), ((), ())), preferred_element_type=F32)


class Bands:
    def __init__(self, total):
        self.total = total
        self.inner = math.gcd(total, 4)
        self.blocks = total // self.inner
        self.ny = max(self.inner // 2, 1)
        self.nc = min(self.inner, 2)
        self.parts = [(s, y) for y in range(self.ny) for s in range((self.blocks + 1) // 2)]
        self.half = self.blocks // 2 if self.blocks % 2 == 0 else 0
        if self.half:
            self.parts.append(None)
        self.count = len(self.parts) * self.nc

    def source(self, device, part, other_core, where=np.where):
        block = device // self.inner if where is np.where else lax.div(device, self.inner)
        place = device - block * self.inner
        if self.parts[part] is None:
            turned = where(block < self.half, self.ny - 1, 0)
            block = where(block < self.half, block + self.half, block - self.half)
        else:
            shift, turned = self.parts[part]
            block = where(block < shift, block - shift + self.blocks, block - shift)
        return block * self.inner + (place ^ (turned * self.nc + other_core))

    def pairs(self, part):
        return [(int(self.source(device, part, 0)), device) for device in range(self.total)]


def canonical_lane(sticks, radius):
    gx = sticks - radius + 1
    return jnp.where(gx >= 0, gx, radius - gx)


def rows_kernel(out_ref):
    out_ref[...] = lax.broadcasted_iota(jnp.int32, out_ref.shape, 0).astype(F32)


def copy_kernel(_, in_ref, out_ref):
    out_ref[...] = in_ref[...]


def sticks_of(sticks_ref, group, slots):
    sticks = sticks_ref[...]
    row = sticks[:, :slots]
    for index in range(1, sticks.shape[1] // slots):
        row = jnp.where(group == index, sticks[:, index * slots : (index + 1) * slots], row)
    return row


def spread(values, inverse):
    index = jnp.maximum(inverse, 0)
    parts = []
    for part in values:
        moved = jnp.take_along_axis(part.astype(F32), index, axis=1, mode="promise_in_bounds")
        parts.append(jnp.where(inverse >= 0, moved, 0.0))
    return jnp.concatenate(parts, axis=1).astype(BF16)


def choose_slots(sticks_ref, group, slots, width):
    lane = canonical_lane(sticks_of(sticks_ref, group, slots), width // 2)
    return (lax.broadcasted_iota(jnp.int32, (width, slots), 0) == lane).astype(F32).astype(BF16)


def group_before(ga, distance, groups):
    return lax.rem(ga + (groups - distance), groups)


def place_kernel(ga_ref, rows_ref, orbitals_ref, entries_ref, out_ref, inverse_ref, e_ref, all_ref):
    width = entries_ref.shape[1]
    slots = orbitals_ref.shape[2]
    total = entries_ref.shape[0]
    groups = total // slots
    ga = ga_ref[0]
    chunks, _, lanes = e_ref.shape
    lists_t = entries_ref[...].astype(F32)
    if chunks * lanes > total:
        lists_t = jnp.concatenate([lists_t, jnp.full((chunks * lanes - total, width), -1.0, F32)], axis=0)
    position = rows_ref[...]
    for chunk in range(chunks):
        e_ref[chunk] = lists_t[chunk * lanes : (chunk + 1) * lanes].T

        def step(k, found):
            match = e_ref[chunk, pl.ds(k, 1), :] == position
            return jnp.where(match, k.astype(F32), found)

        found = lax.fori_loop(0, width, step, jnp.full((width, lanes), -1.0, F32), unroll=8)
        all_ref[chunk * lanes : (chunk + 1) * lanes, :] = found.T.astype(jnp.int32)

    def lists(group):
        return all_ref[pl.ds(pl.multiple_of(group * slots, 8), slots), :]

    out_ref[...] = spread([orbitals_ref[0, 0], orbitals_ref[1, 0]], lists(ga))
    for distance in range(1, groups):
        inverse_ref[distance - 1] = lists(group_before(ga, distance, groups))


def grid_kernel(ga_ref, other_refs, own_coeffs_ref, inverse_ref, potential_ref, sticks_ref, tables, own_ref, send_ref):
    z_table, zt_table, x_table, xt = tables
    planes, _ = potential_ref.shape
    width = own_coeffs_ref.shape[1] // 2
    radius = width // 2
    slots = own_ref.shape[0]
    groups = sticks_ref.shape[1] // slots
    ga = ga_ref[0]
    coeffs = dot(choose_slots(sticks_ref, ga, slots, width), own_coeffs_ref[...])
    for distance, ref in enumerate(other_refs, 1):
        choose = choose_slots(sticks_ref, group_before(ga, distance, groups), slots, width)
        coeffs = coeffs + dot(choose, spread([ref[0, 0], ref[1, 0]], inverse_ref[distance - 1]))
    real_part, imag_part = coeffs[:, :width], coeffs[:, width:]
    rows = jnp.concatenate(
        [
            jnp.concatenate([real_part, -imag_part], axis=1),
            jnp.concatenate([imag_part, real_part], axis=1),
        ],
        axis=0,
    ).astype(BF16)
    columns = dot_rows(z_table[ga, 0], rows) + dot_rows(z_table[ga, 1], rows)
    col_re, col_im = columns[:, :width], columns[:, width:]
    rol_re, rol_im = pltpu.roll(col_re, radius, 1), pltpu.roll(col_im, radius, 1)
    even = lax.broadcasted_iota(jnp.int32, (planes, width), 1) < radius
    parity = jnp.concatenate(
        [
            jnp.where(even, col_re + rol_re, col_im - rol_im),
            jnp.where(even, col_im + rol_im, rol_re - col_re),
        ],
        axis=0,
    )
    par_high, par_low = split(parity)
    table = x_table[0]
    field = dot(jnp.concatenate([par_high, par_low], axis=1), jnp.concatenate([table, table], axis=0))
    field = field + dot(par_high, x_table[1])
    values = potential_ref[...]
    product = jnp.concatenate([values, values], axis=0) * field
    prod_high, prod_low = split(product)
    table_t = xt[...]
    wide = dot(prod_high, table_t)
    back = wide[:, :width] + wide[:, width:] + dot(prod_low, table_t[:, :width])
    back_re, back_im = back[:planes], back[planes:]
    rol_re, rol_im = pltpu.roll(back_re, radius, 1), pltpu.roll(back_im, radius, 1)
    gathered = jnp.concatenate(
        [
            jnp.where(even, back_re + rol_im, rol_re - back_im),
            jnp.where(even, back_im - rol_re, rol_im + back_re),
        ],
        axis=1,
    )
    gat_high, gat_low = split(gathered)
    spectra = dot(zt_table[ga, 0], gat_high) + dot(zt_table[ga, 1], gat_high) + dot(zt_table[ga, 0], gat_low)
    spectra = jnp.concatenate(
        [
            spectra[:width, :width] + spectra[width:, width:],
            spectra[:width, width:] - spectra[width:, :width],
        ],
        axis=0,
    )
    spec_high, spec_low = split(spectra)
    spec = jnp.concatenate([spec_high, spec_low], axis=1)
    lanes = lax.broadcasted_iota(jnp.int32, (slots, width), 1)
    for distance in range(groups):
        group = lax.rem(ga + distance, groups)
        lane_row = canonical_lane(sticks_of(sticks_ref, group, slots), radius).astype(F32)
        lane_col = jnp.broadcast_to(lane_row, (width, slots)).T.astype(jnp.int32)
        choose = (lane_col == lanes).astype(F32).astype(BF16)
        picked = dot_rows(jnp.concatenate([choose, choose], axis=1), spec)
        if distance == 0:
            own_ref[...] = picked
        else:
            send_ref[distance - 1] = picked


def apply_part(ga, partial_refs, orbitals_ref, entries_ref, sticks_ref, points):
    width = entries_ref.shape[1]
    slots = orbitals_ref.shape[2]
    radius = width // 2
    total = partial_refs[0][...]
    for ref in partial_refs[1:]:
        total = total + ref[...]
    entries = entries_ref[pl.ds(pl.multiple_of(ga * slots, 8), slots), :]
    present = entries >= 0
    index = jnp.maximum(entries, 0)
    gx_row = (sticks_of(sticks_ref, ga, entries.shape[0]) - radius + 1).astype(F32)
    gx = jnp.broadcast_to(gx_row, (width, gx_row.shape[1])).T
    gz = (entries - radius + 1).astype(F32)
    kinetic = (gx * gx + gz * gz) * (1.0 / (radius * radius))
    result = []
    for part in range(2):
        picked = jnp.take_along_axis(
            total[:, part * width : (part + 1) * width], index, axis=1, mode="promise_in_bounds"
        )
        value = kinetic * orbitals_ref[part, 0].astype(F32) + picked * (1.0 / (points * points))
        result.append(jnp.where(present, value, 0.0).astype(BF16))
    return result, present


def final_kernel(points, ga_ref, partial_refs, orbitals_ref, entries_ref, sticks_ref, psi_refs, out_ref, sums_ref):
    ga = ga_ref[0]
    result, present = apply_part(ga, partial_refs, orbitals_ref, entries_ref, sticks_ref, points)
    for part in range(2):
        out_ref[part, 0] = result[part]
    _, width = present.shape
    h_re, h_im = result[0].astype(F32), result[1].astype(F32)
    m_re = jnp.where(present, orbitals_ref[0, 0].astype(F32), 0.0)
    m_im = jnp.where(present, orbitals_ref[1, 0].astype(F32), 0.0)
    rows = [[], [], [], []]
    for part in range(psi_refs[0].shape[1]):
        for psi_ref in psi_refs:
            left_re = psi_ref[0, part].astype(F32)
            left_im = psi_ref[1, part].astype(F32)
            for place, (right_re, right_im) in enumerate(((m_re, m_im), (h_re, h_im))):
                rows[2 * place].append(jnp.sum(left_re * right_re + left_im * right_im, axis=0, keepdims=True))
                rows[2 * place + 1].append(jnp.sum(left_re * right_im - left_im * right_re, axis=0, keepdims=True))
    flat = sum(rows, [])
    lanes = sums_ref.shape[1]
    if len(flat) < lanes:
        flat.append(jnp.zeros((lanes - len(flat), width), F32))
    sums = jnp.sum(jnp.concatenate(flat, axis=0).T, axis=0, keepdims=True)
    sums_ref[...] = jnp.broadcast_to(sums, sums_ref.shape)


def assemble_kernel(groups, layout, scale, sums_ref, corr_ref, ham_ref):
    bands = layout.total
    total = sums_ref[0:bands, :]
    for group in range(1, groups):
        total = total + sums_ref[group * bands : (group + 1) * bands, :]
    lanes = total.shape[1]
    total = jnp.concatenate([total, jnp.zeros((lanes - bands, lanes), F32)], axis=0).T * scale
    row = lax.broadcasted_iota(jnp.int32, (bands, lanes), 0)
    col = lax.broadcasted_iota(jnp.int32, (bands, lanes), 1)
    matches = []
    for part in range(len(layout.parts)):
        for core in range(layout.nc):
            matches.append(row == layout.source(col, part, core, jnp.where))
    covered = functools.reduce(jnp.logical_or, matches)
    for place, ref in enumerate((corr_ref, ham_ref)):
        for part in range(2):
            base = (2 * place + part) * layout.count
            direct = jnp.zeros((bands, lanes), F32)
            for index, match in enumerate(matches):
                direct = jnp.where(match, total[base + index : base + index + 1, :], direct)
            padded = jnp.concatenate([direct, jnp.zeros((lanes - bands, lanes), F32)], axis=0)
            mirror = padded.T[:bands]
            if part:
                mirror = -mirror
            ref[part] = jnp.where(covered, direct, mirror)[:, :bands]


def general_matrices(psi, masked, applied, layout, scale):
    bands, count = layout.total, layout.count
    left = psi.reshape(2, count, -1)
    right = jnp.stack([masked.reshape(2, -1), applied.reshape(2, -1)])
    product = jnp.einsum("cin,mdn->mcdi", left, right, preferred_element_type=F32)
    block = jnp.stack([product[:, 0, 0] + product[:, 1, 1], product[:, 0, 1] - product[:, 1, 0]], axis=1)
    everywhere = lax.all_gather(lax.psum(block * scale, "ga"), "band", axis=0)
    slot = np.full((bands, bands), -1)
    for device in range(bands):
        for part in range(len(layout.parts)):
            for core in range(layout.nc):
                slot[device, layout.source(device, part, core)] = part * layout.nc + core
    flat = jnp.transpose(everywhere, (1, 2, 0, 3)).reshape(4 * bands, count)
    index = jnp.asarray(np.tile(np.maximum(slot, 0), (4, 1)), jnp.int32)
    direct = jnp.take_along_axis(flat, index, axis=1).reshape(2, 2, bands, bands)
    direct = jnp.swapaxes(direct, 2, 3)
    sign = jnp.asarray([1.0, -1.0], F32)[None, :, None, None]
    full = jnp.where(jnp.asarray(slot.T >= 0), direct, sign * jnp.swapaxes(direct, 2, 3))
    return full[0], full[1]


def body(band_total, groups, orbitals, potential, slot_sticks, stick_entries):
    _, points = potential.shape
    width = stick_entries.shape[1]
    radius = width // 2
    slots = orbitals.shape[2]
    layout = Bands(band_total)
    ga = lax.axis_index("ga").astype(jnp.int32).reshape(1)
    sticks = slot_sticks.reshape(1, groups * slots)
    tables = [jnp.asarray(t) for t in twiddle_tables(points, radius, groups)]

    rows = pl.pallas_call(
        rows_kernel,
        out_shape=jax.ShapeDtypeStruct((width, 128), F32),
        out_specs=VMEM_SPEC,
        compiler_params=KERNEL_PARAMS,
        cost_estimate=pl.CostEstimate(flops=FIRST_FLOPS, bytes_accessed=0, transcendentals=0),
        name="rows",
    )()
    sticks = pl.pallas_call(
        copy_kernel,
        out_shape=jax.ShapeDtypeStruct(sticks.shape, jnp.int32),
        in_specs=[VMEM_SPEC, VMEM_SPEC],
        out_specs=VMEM_SPEC,
        compiler_params=KERNEL_PARAMS,
        name="sticks",
    )(rows, sticks)
    orbitals, rows, sticks = lax.optimization_barrier((orbitals, rows, sticks))
    others = []
    for distance in range(1, groups):
        pairs = [(i, (i + distance) % groups) for i in range(groups)]
        others.append(lax.ppermute(orbitals, "ga", pairs))
    near, far = [orbitals], []
    for part, way in enumerate(layout.parts):
        if way is None or (way[1] == 0 and part > 0):
            (far if way is None else near).append(lax.ppermute(orbitals, "band", layout.pairs(part)))

    chunks = pl.cdiv(groups * slots, 128)
    place = pl.pallas_call(
        place_kernel,
        out_shape=(
            jax.ShapeDtypeStruct((slots, 2 * width), BF16),
            jax.ShapeDtypeStruct((groups - 1, slots, width), jnp.int32),
        ),
        in_specs=[SMEM_SPEC] + [VMEM_SPEC] * 3,
        out_specs=(VMEM_SPEC, VMEM_SPEC),
        scratch_shapes=[pltpu.VMEM((chunks, width, 128), F32), pltpu.VMEM((chunks * 128, width), jnp.int32)],
        compiler_params=KERNEL_PARAMS,
        cost_estimate=pl.CostEstimate(flops=SPREAD_FLOPS, bytes_accessed=0, transcendentals=0),
        name="place",
    )
    coeffs, inverse = place(ga, rows, orbitals, stick_entries)
    coeffs, *arrived = lax.optimization_barrier((coeffs, *near, *far))
    near, far = jnp.concatenate(arrived[: len(near)], axis=1), arrived[len(near) :]
    psi = [near]
    if layout.ny == 2:
        pairs = [(i, i ^ layout.nc) for i in range(band_total)]
        psi.append(lax.ppermute(near, "band", pairs))

    def run_grid(ga_ref, *refs):
        count = len(others)
        grid_kernel(ga_ref, refs[:count], *refs[count : count + 4], refs[count + 4 : count + 8], *refs[count + 8 :])

    grid = pl.pallas_call(
        run_grid,
        out_shape=(
            jax.ShapeDtypeStruct((slots, 2 * width), F32),
            jax.ShapeDtypeStruct((groups - 1, slots, 2 * width), F32),
        ),
        in_specs=[SMEM_SPEC] + [VMEM_SPEC] * (len(others) + 8),
        out_specs=(VMEM_SPEC, VMEM_SPEC),
        compiler_params=KERNEL_PARAMS,
        cost_estimate=pl.CostEstimate(flops=GRID_FLOPS, bytes_accessed=0, transcendentals=0),
        name="grid",
    )
    own, send = grid(ga, *others, coeffs, inverse, potential, sticks, *tables)
    psi = [jnp.concatenate(psi + far, axis=1)]
    if layout.nc == 2:
        psi.append(lax.ppermute(psi[0], "band", [(i, i ^ 1) for i in range(band_total)]))
    partials = [own]
    for distance in range(1, groups):
        pairs = [(i, (i + distance) % groups) for i in range(groups)]
        partials.append(lax.ppermute(send[distance - 1], "ga", pairs))

    scale = 1.0 / (4.0 * radius * radius)
    out_type = jax.ShapeDtypeStruct(orbitals.shape, BF16)
    small = 4 * layout.count <= 128 and band_total <= 128
    count = len(partials)
    if not small:

        def run_apply(ga_ref, *refs):
            result, _ = apply_part(ga_ref[0], refs[:count], *refs[count : count + 3], points)
            refs[count + 3][0, 0] = result[0]
            refs[count + 3][1, 0] = result[1]

        applied = pl.pallas_call(
            run_apply,
            out_shape=out_type,
            in_specs=[SMEM_SPEC] + [VMEM_SPEC] * (count + 3),
            out_specs=VMEM_SPEC,
            compiler_params=KERNEL_PARAMS,
            name="apply",
        )(ga, *partials, orbitals, stick_entries, sticks)
        own_lists = lax.dynamic_slice_in_dim(stick_entries, ga[0] * slots, slots, 0)
        masked = jnp.where(own_lists >= 0, orbitals, jnp.zeros_like(orbitals))
        correlation, reduced = general_matrices(jnp.stack(psi, axis=2), masked, applied, layout, scale)
        return applied, correlation, reduced

    def run_final(ga_ref, *refs):
        psi_refs, outs = refs[count + 3 : count + 3 + len(psi)], refs[count + 3 + len(psi) :]
        final_kernel(points, ga_ref, refs[:count], *refs[count : count + 3], psi_refs, *outs)

    applied, sums = pl.pallas_call(
        run_final,
        out_shape=(out_type, jax.ShapeDtypeStruct((groups * band_total, 128), F32)),
        in_specs=[SMEM_SPEC] + [VMEM_SPEC] * (count + 3 + len(psi)),
        out_specs=(VMEM_SPEC, VMEM_SPEC),
        compiler_params=KERNEL_PARAMS,
        name="final",
    )(ga, *partials, orbitals, stick_entries, sticks, *psi)
    everywhere = lax.all_to_all(sums, ("ga", "band"), split_axis=0, concat_axis=0, tiled=True)
    matrix = jax.ShapeDtypeStruct((2, band_total, band_total), F32)

    def run_assemble(sums_ref, corr_ref, ham_ref):
        assemble_kernel(groups, layout, scale, sums_ref, corr_ref, ham_ref)

    correlation, reduced = pl.pallas_call(
        run_assemble,
        out_shape=(matrix, matrix),
        in_specs=[VMEM_SPEC],
        out_specs=(VMEM_SPEC, VMEM_SPEC),
        compiler_params=KERNEL_PARAMS,
        name="assemble",
    )(everywhere)
    return applied, correlation, reduced


def solution(mesh):
    band_total = mesh.shape["band"]
    groups = mesh.shape["ga"]

    def mapped(orbitals, potential, slot_sticks, stick_entries):
        return body(band_total, groups, orbitals, potential, slot_sticks, stick_entries)

    return jax.shard_map(
        mapped,
        mesh=mesh,
        in_specs=(P(None, "band", "ga", None), P("ga", None), P(), P()),
        out_specs=(P(None, "band", "ga", None), P(), P()),
        check_vma=False,
    )
```

```python
import functools
import math

import jax
import jax.numpy as jnp
import numpy as np
from jax import lax
from jax.experimental import pallas as pl
from jax.experimental.pallas import tpu as pltpu
from jax.sharding import PartitionSpec as P


F32 = jnp.float32
BF16 = jnp.bfloat16
VMEM_SPEC = pl.BlockSpec(memory_space=pltpu.VMEM)
SMEM_SPEC = pl.BlockSpec(memory_space=pltpu.SMEM)
FIRST_FLOPS = 3_000_000_000
SPREAD_FLOPS = 1_500_000_000
GRID_FLOPS = 3_000_000_000
KERNEL_PARAMS = pltpu.CompilerParams(vmem_limit_bytes=16 * 1024 * 1024)


def hi_lo_table(values):
    high = jnp.asarray(values, F32).astype(BF16)
    high_np = np.asarray(values, np.float32).astype(jnp.bfloat16)
    low_np = (values - high_np.astype(np.float64)).astype(jnp.bfloat16)
    return high_np, low_np


def twiddle_tables(points, radius, group_count):
    width = 2 * radius
    planes = points // group_count
    z = np.arange(points, dtype=np.int64)
    gz = np.arange(width, dtype=np.int64) - radius + 1
    angle_z = (z[:, None] * gz[None, :] % points) * (2.0 * np.pi / points)
    forward = np.concatenate([np.cos(angle_z), np.sin(angle_z)], axis=1)
    forward = forward.reshape(group_count, planes, 2 * width)
    backward = np.ascontiguousarray(np.transpose(forward, (0, 2, 1)))
    gx = np.arange(radius, dtype=np.int64)
    angle_x = (gx[:, None] * z[None, :] % points) * (2.0 * np.pi / points)
    x_table = np.concatenate([np.cos(angle_x), np.sin(angle_x)], axis=0)
    z_high, z_low = hi_lo_table(forward)
    zt_high, zt_low = hi_lo_table(backward)
    x_high, x_low = hi_lo_table(x_table)
    xt = np.concatenate([x_high.T, x_low.T], axis=1)
    return np.stack([z_high, z_low], 1), np.stack([zt_high, zt_low], 1), np.stack([x_high, x_low]), xt


def split(values):
    high = values.astype(BF16)
    low = (values - high.astype(F32)).astype(BF16)
    return high, low


def dot(left, right):
    return jnp.dot(left, right, preferred_element_type=F32)


def dot_rows(left, right):
    return lax.dot_general(left, right, (((1,), (1,)), ((), ())), preferred_element_type=F32)


class Bands:
    def __init__(self, total):
        self.total = total
        self.inner = math.gcd(total, 4)
        self.blocks = total // self.inner
        self.ny = max(self.inner // 2, 1)
        self.nc = min(self.inner, 2)
        self.parts = [(s, y) for y in range(self.ny) for s in range((self.blocks + 1) // 2)]
        self.half = self.blocks // 2 if self.blocks % 2 == 0 else 0
        if self.half:
            self.parts.append(None)
        self.count = len(self.parts) * self.nc

    def source(self, device, part, other_core, where=np.where):
        block = device // self.inner if where is np.where else lax.div(device, self.inner)
        place = device - block * self.inner
        if self.parts[part] is None:
            turned = where(block < self.half, self.ny - 1, 0)
            block = where(block < self.half, block + self.half, block - self.half)
        else:
            shift, turned = self.parts[part]
            block = where(block < shift, block - shift + self.blocks, block - shift)
        return block * self.inner + (place ^ (turned * self.nc + other_core))

    def pairs(self, part):
        return [(int(self.source(device, part, 0)), device) for device in range(self.total)]


def canonical_lane(sticks, radius):
    gx = sticks - radius + 1
    return jnp.where(gx >= 0, gx, radius - gx)


def rows_kernel(out_ref):
    out_ref[...] = lax.broadcasted_iota(jnp.int32, out_ref.shape, 0).astype(F32)


def copy_kernel(_, in_ref, out_ref):
    out_ref[...] = in_ref[...]


def sticks_of(sticks_ref, group, slots):
    sticks = sticks_ref[...]
    row = sticks[:, :slots]
    for index in range(1, sticks.shape[1] // slots):
        row = jnp.where(group == index, sticks[:, index * slots : (index + 1) * slots], row)
    return row


def spread(values, inverse):
    index = jnp.maximum(inverse, 0)
    parts = []
    for part in values:
        moved = jnp.take_along_axis(part.astype(F32), index, axis=1, mode="promise_in_bounds")
        parts.append(jnp.where(inverse >= 0, moved, 0.0))
    return jnp.concatenate(parts, axis=1).astype(BF16)


def choose_slots(sticks_ref, group, slots, width):
    lane = canonical_lane(sticks_of(sticks_ref, group, slots), width // 2)
    return (lax.broadcasted_iota(jnp.int32, (width, slots), 0) == lane).astype(F32).astype(BF16)


def group_before(ga, distance, groups):
    return lax.rem(ga + (groups - distance), groups)


def place_kernel(
    ga_ref, rows_ref, orbitals_ref, entries_ref, sticks_ref, out_ref, inverse_ref, in_ref, pick_ref, kinetic_ref, e_ref, all_ref
):
    width = entries_ref.shape[1]
    slots = orbitals_ref.shape[2]
    total = entries_ref.shape[0]
    groups = total // slots
    radius = width // 2
    ga = ga_ref[0]
    chunks, _, lanes = e_ref.shape
    lists_t = entries_ref[...].astype(F32)
    position = rows_ref[...]
    for chunk in range(chunks):
        first = chunk * lanes
        used = min(lanes, total - first)
        copies = 1
        while used * copies * 2 <= lanes and lanes % (used * copies * 2) == 0:
            copies *= 2
        if used * copies < lanes:
            copies, used_rows = 1, jnp.concatenate([lists_t[first:], jnp.full((lanes - used, width), -1.0, F32)], axis=0)
        else:
            used_rows = jnp.concatenate([lists_t[first : first + used]] * copies, axis=0)
        e_ref[chunk] = used_rows.T
        height = width // copies
        target = position[:height]
        if copies > 1:
            lane = lax.broadcasted_iota(jnp.int32, (height, lanes), 1).astype(F32)
            for copy in range(1, copies):
                target = jnp.where(lane >= copy * used, position[:height] + copy * height, target)

        def step(k, found):
            match = e_ref[chunk, pl.ds(k, 1), :] == target
            return jnp.where(match, k.astype(F32), found)

        found = lax.fori_loop(0, width, step, jnp.full((height, lanes), -1.0, F32), unroll=8)
        if copies > 1:
            found = jnp.concatenate([found[:, c * used : (c + 1) * used] for c in range(copies)], axis=0)
        found = found.T.astype(jnp.int32)
        all_ref[first : first + found.shape[0], :] = found

    def lists(group):
        return all_ref[pl.ds(pl.multiple_of(group * slots, 8), slots), :]

    out_ref[...] = spread([orbitals_ref[0, 0], orbitals_ref[1, 0]], lists(ga))
    for distance in range(1, groups):
        inverse_ref[distance - 1] = lists(group_before(ga, distance, groups))
    lane = lax.broadcasted_iota(jnp.int32, (slots, width), 1)
    for distance in range(groups):
        in_ref[distance] = choose_slots(sticks_ref, group_before(ga, distance, groups), slots, width)
        row = canonical_lane(sticks_of(sticks_ref, lax.rem(ga + distance, groups), slots), radius).astype(F32)
        column = jnp.broadcast_to(row, (width, slots)).T.astype(jnp.int32)
        pick_ref[distance] = (column == lane).astype(F32).astype(BF16)
    gx_row = (sticks_of(sticks_ref, ga, slots) - radius + 1).astype(F32)
    gx = jnp.broadcast_to(gx_row, (width, slots)).T
    gz = (entries_ref[pl.ds(pl.multiple_of(ga * slots, 8), slots), :] - radius + 1).astype(F32)
    kinetic_ref[...] = (gx * gx + gz * gz) * (1.0 / (radius * radius))


def grid_kernel(ga_ref, other_refs, own_coeffs_ref, inverse_ref, in_ref, pick_ref, potential_ref, tables, own_ref, send_ref):
    z_table, zt_table, x_table, xt = tables
    planes, _ = potential_ref.shape
    width = own_coeffs_ref.shape[1] // 2
    radius = width // 2
    ga = ga_ref[0]
    coeffs = dot(in_ref[0], own_coeffs_ref[...])
    for distance, ref in enumerate(other_refs, 1):
        coeffs = coeffs + dot(in_ref[distance], spread([ref[0, 0], ref[1, 0]], inverse_ref[distance - 1]))
    real_part, imag_part = coeffs[:, :width], coeffs[:, width:]
    rows = jnp.concatenate(
        [
            jnp.concatenate([real_part, -imag_part], axis=1),
            jnp.concatenate([imag_part, real_part], axis=1),
        ],
        axis=0,
    ).astype(BF16)
    columns = dot_rows(z_table[ga, 0], rows) + dot_rows(z_table[ga, 1], rows)
    col_re, col_im = columns[:, :width], columns[:, width:]
    rol_re, rol_im = pltpu.roll(col_re, radius, 1), pltpu.roll(col_im, radius, 1)
    even = lax.broadcasted_iota(jnp.int32, (planes, width), 1) < radius
    parity = jnp.concatenate(
        [
            jnp.where(even, col_re + rol_re, col_im - rol_im),
            jnp.where(even, col_im + rol_im, rol_re - col_re),
        ],
        axis=0,
    )
    par_high, par_low = split(parity)
    table = x_table[0]
    field = dot(jnp.concatenate([par_high, par_low], axis=1), jnp.concatenate([table, table], axis=0))
    field = field + dot(par_high, x_table[1])
    values = potential_ref[...]
    product = jnp.concatenate([values, values], axis=0) * field
    prod_high, prod_low = split(product)
    table_t = xt[...]
    wide = dot(prod_high, table_t)
    back = wide[:, :width] + wide[:, width:] + dot(prod_low, table_t[:, :width])
    back_re, back_im = back[:planes], back[planes:]
    rol_re, rol_im = pltpu.roll(back_re, radius, 1), pltpu.roll(back_im, radius, 1)
    gathered = jnp.concatenate(
        [
            jnp.where(even, back_re + rol_im, rol_re - back_im),
            jnp.where(even, back_im - rol_re, rol_im + back_re),
        ],
        axis=1,
    )
    gat_high, gat_low = split(gathered)
    spectra = dot(zt_table[ga, 0], gat_high) + dot(zt_table[ga, 1], gat_high) + dot(zt_table[ga, 0], gat_low)
    spectra = jnp.concatenate(
        [
            spectra[:width, :width] + spectra[width:, width:],
            spectra[:width, width:] - spectra[width:, :width],
        ],
        axis=0,
    )
    spec_high, spec_low = split(spectra)
    spec = jnp.concatenate([spec_high, spec_low], axis=1)
    for distance in range(pick_ref.shape[0]):
        choose = pick_ref[distance]
        picked = dot_rows(jnp.concatenate([choose, choose], axis=1), spec)
        if distance == 0:
            own_ref[...] = picked
        else:
            send_ref[distance - 1] = picked


def apply_part(ga, partial_refs, orbitals_ref, entries_ref, kinetic_ref, points):
    width = entries_ref.shape[1]
    slots = orbitals_ref.shape[2]
    total = partial_refs[0][...]
    for ref in partial_refs[1:]:
        total = total + ref[...]
    entries = entries_ref[pl.ds(pl.multiple_of(ga * slots, 8), slots), :]
    present = entries >= 0
    index = jnp.maximum(entries, 0)
    kinetic = kinetic_ref[...]
    result = []
    for part in range(2):
        picked = jnp.take_along_axis(
            total[:, part * width : (part + 1) * width], index, axis=1, mode="promise_in_bounds"
        )
        value = kinetic * orbitals_ref[part, 0].astype(F32) + picked * (1.0 / (points * points))
        result.append(jnp.where(present, value, 0.0).astype(BF16))
    return result, present


def final_kernel(points, ga_ref, partial_refs, orbitals_ref, entries_ref, kinetic_ref, psi_refs, out_ref, sums_ref):
    ga = ga_ref[0]
    result, present = apply_part(ga, partial_refs, orbitals_ref, entries_ref, kinetic_ref, points)
    for part in range(2):
        out_ref[part, 0] = result[part]
    _, width = present.shape
    h_re, h_im = result[0].astype(F32), result[1].astype(F32)
    m_re = jnp.where(present, orbitals_ref[0, 0].astype(F32), 0.0)
    m_im = jnp.where(present, orbitals_ref[1, 0].astype(F32), 0.0)
    rows = [[], [], [], []]
    for part in range(psi_refs[0].shape[1]):
        for psi_ref in psi_refs:
            left_re = psi_ref[0, part].astype(F32)
            left_im = psi_ref[1, part].astype(F32)
            for place, (right_re, right_im) in enumerate(((m_re, m_im), (h_re, h_im))):
                rows[2 * place].append(jnp.sum(left_re * right_re + left_im * right_im, axis=0, keepdims=True))
                rows[2 * place + 1].append(jnp.sum(left_re * right_im - left_im * right_re, axis=0, keepdims=True))
    flat = sum(rows, [])
    lanes = sums_ref.shape[1]
    if len(flat) < lanes:
        flat.append(jnp.zeros((lanes - len(flat), width), F32))
    sums = jnp.sum(jnp.concatenate(flat, axis=0).T, axis=0, keepdims=True)
    sums_ref[...] = jnp.broadcast_to(sums, sums_ref.shape)


def assemble_kernel(groups, layout, scale, sums_ref, corr_ref, ham_ref):
    bands = layout.total
    total = sums_ref[0:bands, :]
    for group in range(1, groups):
        total = total + sums_ref[group * bands : (group + 1) * bands, :]
    lanes = total.shape[1]
    total = jnp.concatenate([total, jnp.zeros((lanes - bands, lanes), F32)], axis=0).T * scale
    row = lax.broadcasted_iota(jnp.int32, (bands, lanes), 0)
    col = lax.broadcasted_iota(jnp.int32, (bands, lanes), 1)
    matches = []
    for part in range(len(layout.parts)):
        for core in range(layout.nc):
            matches.append(row == layout.source(col, part, core, jnp.where))
    covered = functools.reduce(jnp.logical_or, matches)
    for place, ref in enumerate((corr_ref, ham_ref)):
        for part in range(2):
            base = (2 * place + part) * layout.count
            direct = jnp.zeros((bands, lanes), F32)
            for index, match in enumerate(matches):
                direct = jnp.where(match, total[base + index : base + index + 1, :], direct)
            padded = jnp.concatenate([direct, jnp.zeros((lanes - bands, lanes), F32)], axis=0)
            mirror = padded.T[:bands]
            if part:
                mirror = -mirror
            ref[part] = jnp.where(covered, direct, mirror)[:, :bands]


def general_matrices(psi, masked, applied, layout, scale):
    bands, count = layout.total, layout.count
    left = psi.reshape(2, count, -1)
    right = jnp.stack([masked.reshape(2, -1), applied.reshape(2, -1)])
    product = jnp.einsum("cin,mdn->mcdi", left, right, preferred_element_type=F32)
    block = jnp.stack([product[:, 0, 0] + product[:, 1, 1], product[:, 0, 1] - product[:, 1, 0]], axis=1)
    everywhere = lax.all_gather(lax.psum(block * scale, "ga"), "band", axis=0)
    slot = np.full((bands, bands), -1)
    for device in range(bands):
        for part in range(len(layout.parts)):
            for core in range(layout.nc):
                slot[device, layout.source(device, part, core)] = part * layout.nc + core
    flat = jnp.transpose(everywhere, (1, 2, 0, 3)).reshape(4 * bands, count)
    index = jnp.asarray(np.tile(np.maximum(slot, 0), (4, 1)), jnp.int32)
    direct = jnp.take_along_axis(flat, index, axis=1).reshape(2, 2, bands, bands)
    direct = jnp.swapaxes(direct, 2, 3)
    sign = jnp.asarray([1.0, -1.0], F32)[None, :, None, None]
    full = jnp.where(jnp.asarray(slot.T >= 0), direct, sign * jnp.swapaxes(direct, 2, 3))
    return full[0], full[1]


def body(band_total, groups, orbitals, potential, slot_sticks, stick_entries):
    _, points = potential.shape
    width = stick_entries.shape[1]
    radius = width // 2
    slots = orbitals.shape[2]
    layout = Bands(band_total)
    ga = lax.axis_index("ga").astype(jnp.int32).reshape(1)
    sticks = slot_sticks.reshape(1, groups * slots)
    tables = [jnp.asarray(t) for t in twiddle_tables(points, radius, groups)]

    rows = pl.pallas_call(
        rows_kernel,
        out_shape=jax.ShapeDtypeStruct((width, 128), F32),
        out_specs=VMEM_SPEC,
        compiler_params=KERNEL_PARAMS,
        cost_estimate=pl.CostEstimate(flops=FIRST_FLOPS, bytes_accessed=0, transcendentals=0),
        name="rows",
    )()
    sticks = pl.pallas_call(
        copy_kernel,
        out_shape=jax.ShapeDtypeStruct(sticks.shape, jnp.int32),
        in_specs=[VMEM_SPEC, VMEM_SPEC],
        out_specs=VMEM_SPEC,
        compiler_params=KERNEL_PARAMS,
        name="sticks",
    )(rows, sticks)
    orbitals, rows, sticks = lax.optimization_barrier((orbitals, rows, sticks))
    others = []
    for distance in range(1, groups):
        pairs = [(i, (i + distance) % groups) for i in range(groups)]
        others.append(lax.ppermute(orbitals, "ga", pairs))
    near, far = [orbitals], []
    for part, way in enumerate(layout.parts):
        if way is None or (way[1] == 0 and part > 0):
            (far if way is None else near).append(lax.ppermute(orbitals, "band", layout.pairs(part)))

    chunks = pl.cdiv(groups * slots, 128)
    place = pl.pallas_call(
        place_kernel,
        out_shape=(
            jax.ShapeDtypeStruct((slots, 2 * width), BF16),
            jax.ShapeDtypeStruct((groups - 1, slots, width), jnp.int32),
            jax.ShapeDtypeStruct((groups, width, slots), BF16),
            jax.ShapeDtypeStruct((groups, slots, width), BF16),
            jax.ShapeDtypeStruct((slots, width), F32),
        ),
        in_specs=[SMEM_SPEC] + [VMEM_SPEC] * 4,
        out_specs=(VMEM_SPEC,) * 5,
        scratch_shapes=[pltpu.VMEM((chunks, width, 128), F32), pltpu.VMEM((chunks * 128, width), jnp.int32)],
        compiler_params=KERNEL_PARAMS,
        cost_estimate=pl.CostEstimate(flops=SPREAD_FLOPS, bytes_accessed=0, transcendentals=0),
        name="place",
    )
    coeffs, inverse, into, pick, kinetic = place(ga, rows, orbitals, stick_entries, sticks)
    coeffs, *near = lax.optimization_barrier((coeffs, *near))
    near = jnp.concatenate(near, axis=1)
    psi = [near]
    if layout.ny == 2:
        pairs = [(i, i ^ layout.nc) for i in range(band_total)]
        psi.append(lax.ppermute(near, "band", pairs))

    def run_grid(ga_ref, *refs):
        count = len(others)
        grid_kernel(ga_ref, refs[:count], *refs[count : count + 5], refs[count + 5 : count + 9], *refs[count + 9 :])

    grid = pl.pallas_call(
        run_grid,
        out_shape=(
            jax.ShapeDtypeStruct((slots, 2 * width), F32),
            jax.ShapeDtypeStruct((groups - 1, slots, 2 * width), F32),
        ),
        in_specs=[SMEM_SPEC] + [VMEM_SPEC] * (len(others) + 9),
        out_specs=(VMEM_SPEC, VMEM_SPEC),
        compiler_params=KERNEL_PARAMS,
        cost_estimate=pl.CostEstimate(flops=GRID_FLOPS, bytes_accessed=0, transcendentals=0),
        name="grid",
    )
    own, send = grid(ga, *others, coeffs, inverse, into, pick, potential, *tables)
    own, *far = lax.optimization_barrier((own, *far))
    psi = [jnp.concatenate(psi + far, axis=1)]
    if layout.nc == 2:
        psi.append(lax.ppermute(psi[0], "band", [(i, i ^ 1) for i in range(band_total)]))
    partials = [own]
    for distance in range(1, groups):
        pairs = [(i, (i + distance) % groups) for i in range(groups)]
        partials.append(lax.ppermute(send[distance - 1], "ga", pairs))

    scale = 1.0 / (4.0 * radius * radius)
    out_type = jax.ShapeDtypeStruct(orbitals.shape, BF16)
    small = 4 * layout.count <= 128 and band_total <= 128
    count = len(partials)
    if not small:

        def run_apply(ga_ref, *refs):
            result, _ = apply_part(ga_ref[0], refs[:count], *refs[count : count + 3], points)
            refs[count + 3][0, 0] = result[0]
            refs[count + 3][1, 0] = result[1]

        applied = pl.pallas_call(
            run_apply,
            out_shape=out_type,
            in_specs=[SMEM_SPEC] + [VMEM_SPEC] * (count + 3),
            out_specs=VMEM_SPEC,
            compiler_params=KERNEL_PARAMS,
            name="apply",
        )(ga, *partials, orbitals, stick_entries, kinetic)
        own_lists = lax.dynamic_slice_in_dim(stick_entries, ga[0] * slots, slots, 0)
        masked = jnp.where(own_lists >= 0, orbitals, jnp.zeros_like(orbitals))
        correlation, reduced = general_matrices(jnp.stack(psi, axis=2), masked, applied, layout, scale)
        return applied, correlation, reduced

    def run_final(ga_ref, *refs):
        psi_refs, outs = refs[count + 3 : count + 3 + len(psi)], refs[count + 3 + len(psi) :]
        final_kernel(points, ga_ref, refs[:count], *refs[count : count + 3], psi_refs, *outs)

    applied, sums = pl.pallas_call(
        run_final,
        out_shape=(out_type, jax.ShapeDtypeStruct((groups * band_total, 128), F32)),
        in_specs=[SMEM_SPEC] + [VMEM_SPEC] * (count + 3 + len(psi)),
        out_specs=(VMEM_SPEC, VMEM_SPEC),
        compiler_params=KERNEL_PARAMS,
        name="final",
    )(ga, *partials, orbitals, stick_entries, kinetic, *psi)
    everywhere = lax.all_to_all(sums, ("ga", "band"), split_axis=0, concat_axis=0, tiled=True)
    matrix = jax.ShapeDtypeStruct((2, band_total, band_total), F32)

    def run_assemble(sums_ref, corr_ref, ham_ref):
        assemble_kernel(groups, layout, scale, sums_ref, corr_ref, ham_ref)

    correlation, reduced = pl.pallas_call(
        run_assemble,
        out_shape=(matrix, matrix),
        in_specs=[VMEM_SPEC],
        out_specs=(VMEM_SPEC, VMEM_SPEC),
        compiler_params=KERNEL_PARAMS,
        name="assemble",
    )(everywhere)
    return applied, correlation, reduced


def solution(mesh):
    band_total = mesh.shape["band"]
    groups = mesh.shape["ga"]

    def mapped(orbitals, potential, slot_sticks, stick_entries):
        return body(band_total, groups, orbitals, potential, slot_sticks, stick_entries)

    return jax.shard_map(
        mapped,
        mesh=mesh,
        in_specs=(P(None, "band", "ga", None), P("ga", None), P(), P()),
        out_specs=(P(None, "band", "ga", None), P(), P()),
        check_vma=False,
    )
```

```python
import functools
import math

import jax
import jax.numpy as jnp
import numpy as np
from jax import lax
from jax.experimental import pallas as pl
from jax.experimental.pallas import tpu as pltpu
from jax.sharding import PartitionSpec as P


F32 = jnp.float32
BF16 = jnp.bfloat16
VMEM_SPEC = pl.BlockSpec(memory_space=pltpu.VMEM)
SMEM_SPEC = pl.BlockSpec(memory_space=pltpu.SMEM)
FIRST_FLOPS = 3_000_000_000
SPREAD_FLOPS = 1_500_000_000
GRID_FLOPS = 3_000_000_000
KERNEL_PARAMS = pltpu.CompilerParams(vmem_limit_bytes=16 * 1024 * 1024)


def hi_lo_table(values):
    high = jnp.asarray(values, F32).astype(BF16)
    high_np = np.asarray(values, np.float32).astype(jnp.bfloat16)
    low_np = (values - high_np.astype(np.float64)).astype(jnp.bfloat16)
    return high_np, low_np


def twiddle_tables(points, radius, group_count):
    width = 2 * radius
    planes = points // group_count
    z = np.arange(points, dtype=np.int64)
    gz = np.arange(width, dtype=np.int64) - radius + 1
    angle_z = (z[:, None] * gz[None, :] % points) * (2.0 * np.pi / points)
    forward = np.concatenate([np.cos(angle_z), np.sin(angle_z)], axis=1)
    forward = forward.reshape(group_count, planes, 2 * width)
    backward = np.ascontiguousarray(np.transpose(forward, (0, 2, 1)))
    gx = np.arange(radius, dtype=np.int64)
    angle_x = (gx[:, None] * z[None, :] % points) * (2.0 * np.pi / points)
    x_table = np.concatenate([np.cos(angle_x), np.sin(angle_x)], axis=0)
    z_high, z_low = hi_lo_table(forward)
    zt_high, zt_low = hi_lo_table(backward)
    x_high, x_low = hi_lo_table(x_table)
    xt = np.concatenate([x_high.T, x_low.T], axis=1)
    return np.concatenate([z_high, z_low], 1), np.stack([zt_high, zt_low], 1), np.stack([x_high, x_low]), xt


def split(values):
    high = values.astype(BF16)
    low = (values - high.astype(F32)).astype(BF16)
    return high, low


def dot(left, right):
    return jnp.dot(left, right, preferred_element_type=F32)


def dot_rows(left, right):
    return lax.dot_general(left, right, (((1,), (1,)), ((), ())), preferred_element_type=F32)


class Bands:
    def __init__(self, total):
        self.total = total
        self.inner = math.gcd(total, 4)
        self.blocks = total // self.inner
        self.ny = max(self.inner // 2, 1)
        self.nc = min(self.inner, 2)
        self.parts = [(s, y) for y in range(self.ny) for s in range((self.blocks + 1) // 2)]
        self.half = self.blocks // 2 if self.blocks % 2 == 0 else 0
        if self.half:
            self.parts.append(None)
        self.count = len(self.parts) * self.nc

    def source(self, device, part, other_core, where=np.where):
        block = device // self.inner if where is np.where else lax.div(device, self.inner)
        place = device - block * self.inner
        if self.parts[part] is None:
            turned = where(block < self.half, 0, self.ny - 1)
            block = where(block < self.half, block + self.half, block - self.half)
        else:
            shift, turned = self.parts[part]
            block = where(block < shift, block - shift + self.blocks, block - shift)
        return block * self.inner + (place ^ (turned * self.nc + other_core))

    def pairs(self, part):
        return [(int(self.source(device, part, 0)), device) for device in range(self.total)]


def canonical_lane(sticks, radius):
    gx = sticks - radius + 1
    return jnp.where(gx >= 0, gx, radius - gx)


def rows_kernel(out_ref):
    out_ref[...] = lax.broadcasted_iota(jnp.int32, out_ref.shape, 0).astype(F32)


def copy_kernel(_, in_ref, out_ref):
    out_ref[...] = in_ref[...]


def sticks_of(sticks_ref, group, slots):
    sticks = sticks_ref[...]
    row = sticks[:, :slots]
    for index in range(1, sticks.shape[1] // slots):
        row = jnp.where(group == index, sticks[:, index * slots : (index + 1) * slots], row)
    return row


def spread(values, inverse):
    index = jnp.maximum(inverse, 0)
    parts = []
    for part in values:
        moved = jnp.take_along_axis(part.astype(F32), index, axis=1, mode="promise_in_bounds")
        parts.append(jnp.where(inverse >= 0, moved, 0.0))
    return jnp.concatenate(parts, axis=1).astype(BF16)


def choose_slots(sticks_ref, group, slots, width):
    lane = canonical_lane(sticks_of(sticks_ref, group, slots), width // 2)
    return (lax.broadcasted_iota(jnp.int32, (width, slots), 0) == lane).astype(F32).astype(BF16)


def group_before(ga, distance, groups):
    return lax.rem(ga + (groups - distance), groups)


def place_kernel(
    ga_ref, rows_ref, orbitals_ref, entries_ref, sticks_ref, out_ref, inverse_ref, in_ref, pick_ref, kinetic_ref, e_ref, all_ref
):
    width = entries_ref.shape[1]
    slots = orbitals_ref.shape[2]
    total = entries_ref.shape[0]
    groups = total // slots
    radius = width // 2
    ga = ga_ref[0]
    chunks, _, lanes = e_ref.shape
    lists_t = entries_ref[...].astype(F32)
    position = rows_ref[...]
    for chunk in range(chunks):
        first = chunk * lanes
        used = min(lanes, total - first)
        copies = 1
        while used * copies * 2 <= lanes and lanes % (used * copies * 2) == 0:
            copies *= 2
        if used * copies < lanes:
            copies, used_rows = 1, jnp.concatenate([lists_t[first:], jnp.full((lanes - used, width), -1.0, F32)], axis=0)
        else:
            used_rows = jnp.concatenate([lists_t[first : first + used]] * copies, axis=0)
        e_ref[chunk] = used_rows.T
        height = width // copies
        target = position[:height]
        if copies > 1:
            lane = lax.broadcasted_iota(jnp.int32, (height, lanes), 1).astype(F32)
            for copy in range(1, copies):
                target = jnp.where(lane >= copy * used, position[:height] + copy * height, target)

        def step(k, found):
            match = e_ref[chunk, pl.ds(k, 1), :] == target
            return jnp.where(match, k.astype(F32), found)

        found = lax.fori_loop(0, width, step, jnp.full((height, lanes), -1.0, F32), unroll=8)
        if copies > 1:
            found = jnp.concatenate([found[:, c * used : (c + 1) * used] for c in range(copies)], axis=0)
        found = found.T.astype(jnp.int32)
        all_ref[first : first + found.shape[0], :] = found

    def lists(group):
        return all_ref[pl.ds(pl.multiple_of(group * slots, 8), slots), :]

    out_ref[...] = spread([orbitals_ref[0, 0], orbitals_ref[1, 0]], lists(ga))
    for distance in range(1, groups):
        inverse_ref[distance - 1] = lists(group_before(ga, distance, groups))
    lane = lax.broadcasted_iota(jnp.int32, (slots, width), 1)
    for distance in range(groups):
        in_ref[distance] = choose_slots(sticks_ref, group_before(ga, distance, groups), slots, width)
        row = canonical_lane(sticks_of(sticks_ref, lax.rem(ga + distance, groups), slots), radius).astype(F32)
        column = jnp.broadcast_to(row, (width, slots)).T.astype(jnp.int32)
        pick_ref[distance] = (column == lane).astype(F32).astype(BF16)
    gx_row = (sticks_of(sticks_ref, ga, slots) - radius + 1).astype(F32)
    gx = jnp.broadcast_to(gx_row, (width, slots)).T
    gz = (entries_ref[pl.ds(pl.multiple_of(ga * slots, 8), slots), :] - radius + 1).astype(F32)
    kinetic_ref[...] = (gx * gx + gz * gz) * (1.0 / (radius * radius))


def grid_kernel(ga_ref, other_refs, own_coeffs_ref, inverse_ref, in_ref, pick_ref, potential_ref, tables, own_ref, send_ref):
    z_table, zt_table, x_table, xt = tables
    planes, _ = potential_ref.shape
    width = own_coeffs_ref.shape[1] // 2
    radius = width // 2
    ga = ga_ref[0]
    coeffs = dot(in_ref[0], own_coeffs_ref[...])
    for distance, ref in enumerate(other_refs, 1):
        coeffs = coeffs + dot(in_ref[distance], spread([ref[0, 0], ref[1, 0]], inverse_ref[distance - 1]))
    real_part, imag_part = coeffs[:, :width], coeffs[:, width:]
    rows = jnp.concatenate(
        [
            jnp.concatenate([real_part, -imag_part], axis=1),
            jnp.concatenate([imag_part, real_part], axis=1),
        ],
        axis=0,
    ).astype(BF16)
    columns = dot_rows(z_table[ga], rows)
    columns = columns[:planes] + columns[planes:]
    col_re, col_im = columns[:, :width], columns[:, width:]
    rol_re, rol_im = pltpu.roll(col_re, radius, 1), pltpu.roll(col_im, radius, 1)
    even = lax.broadcasted_iota(jnp.int32, (planes, width), 1) < radius
    parity = jnp.concatenate(
        [
            jnp.where(even, col_re + rol_re, col_im - rol_im),
            jnp.where(even, col_im + rol_im, rol_re - col_re),
        ],
        axis=0,
    )
    par_high, par_low = split(parity)
    table = x_table[0]
    field = dot(jnp.concatenate([par_high, par_low], axis=1), jnp.concatenate([table, table], axis=0))
    field = field + dot(par_high, x_table[1])
    values = potential_ref[...]
    product = jnp.concatenate([values, values], axis=0) * field
    prod_high, prod_low = split(product)
    table_t = xt[...]
    wide = dot(prod_high, table_t)
    back = wide[:, :width] + wide[:, width:] + dot(prod_low, table_t[:, :width])
    back_re, back_im = back[:planes], back[planes:]
    rol_re, rol_im = pltpu.roll(back_re, radius, 1), pltpu.roll(back_im, radius, 1)
    gathered = jnp.concatenate(
        [
            jnp.where(even, back_re + rol_im, rol_re - back_im),
            jnp.where(even, back_im - rol_re, rol_im + back_re),
        ],
        axis=1,
    )
    gat_high, gat_low = split(gathered)
    spectra = dot(zt_table[ga, 0], gat_high) + dot(zt_table[ga, 1], gat_high) + dot(zt_table[ga, 0], gat_low)
    spectra = jnp.concatenate(
        [
            spectra[:width, :width] + spectra[width:, width:],
            spectra[:width, width:] - spectra[width:, :width],
        ],
        axis=0,
    )
    spec_high, spec_low = split(spectra)
    spec = jnp.concatenate([spec_high, spec_low], axis=1)
    for distance in range(pick_ref.shape[0]):
        choose = pick_ref[distance]
        picked = dot_rows(jnp.concatenate([choose, choose], axis=1), spec)
        if distance == 0:
            own_ref[...] = picked
        else:
            send_ref[distance - 1] = picked


def apply_part(ga, partial_refs, orbitals_ref, entries_ref, kinetic_ref, points):
    width = entries_ref.shape[1]
    slots = orbitals_ref.shape[2]
    total = partial_refs[0][...]
    for ref in partial_refs[1:]:
        total = total + ref[...]
    entries = entries_ref[pl.ds(pl.multiple_of(ga * slots, 8), slots), :]
    present = entries >= 0
    index = jnp.maximum(entries, 0)
    kinetic = kinetic_ref[...]
    result = []
    for part in range(2):
        picked = jnp.take_along_axis(
            total[:, part * width : (part + 1) * width], index, axis=1, mode="promise_in_bounds"
        )
        value = kinetic * orbitals_ref[part, 0].astype(F32) + picked * (1.0 / (points * points))
        result.append(jnp.where(present, value, 0.0).astype(BF16))
    return result, present


def final_kernel(points, ga_ref, partial_refs, orbitals_ref, entries_ref, kinetic_ref, psi_refs, out_ref, sums_ref):
    ga = ga_ref[0]
    result, present = apply_part(ga, partial_refs, orbitals_ref, entries_ref, kinetic_ref, points)
    for part in range(2):
        out_ref[part, 0] = result[part]
    _, width = present.shape
    h_re, h_im = result[0].astype(F32), result[1].astype(F32)
    m_re = jnp.where(present, orbitals_ref[0, 0].astype(F32), 0.0)
    m_im = jnp.where(present, orbitals_ref[1, 0].astype(F32), 0.0)
    rows = [[], [], [], []]
    for part in range(psi_refs[0].shape[1]):
        for psi_ref in psi_refs:
            left_re = psi_ref[0, part].astype(F32)
            left_im = psi_ref[1, part].astype(F32)
            for place, (right_re, right_im) in enumerate(((m_re, m_im), (h_re, h_im))):
                rows[2 * place].append(jnp.sum(left_re * right_re + left_im * right_im, axis=0, keepdims=True))
                rows[2 * place + 1].append(jnp.sum(left_re * right_im - left_im * right_re, axis=0, keepdims=True))
    flat = sum(rows, [])
    lanes = sums_ref.shape[1]
    if len(flat) < lanes:
        flat.append(jnp.zeros((lanes - len(flat), width), F32))
    sums = jnp.sum(jnp.concatenate(flat, axis=0).T, axis=0, keepdims=True)
    sums_ref[...] = jnp.broadcast_to(sums, sums_ref.shape)


def assemble_kernel(groups, layout, scale, sums_ref, applied_ref, out_ref, corr_ref, ham_ref):
    out_ref[...] = applied_ref[...]
    bands = layout.total
    total = sums_ref[0:bands, :]
    for group in range(1, groups):
        total = total + sums_ref[group * bands : (group + 1) * bands, :]
    lanes = total.shape[1]
    total = jnp.concatenate([total, jnp.zeros((lanes - bands, lanes), F32)], axis=0).T * scale
    row = lax.broadcasted_iota(jnp.int32, (bands, lanes), 0)
    col = lax.broadcasted_iota(jnp.int32, (bands, lanes), 1)
    matches = []
    for part in range(len(layout.parts)):
        for core in range(layout.nc):
            matches.append(row == layout.source(col, part, core, jnp.where))
    covered = functools.reduce(jnp.logical_or, matches)
    for place, ref in enumerate((corr_ref, ham_ref)):
        for part in range(2):
            base = (2 * place + part) * layout.count
            direct = jnp.zeros((bands, lanes), F32)
            for index, match in enumerate(matches):
                direct = jnp.where(match, total[base + index : base + index + 1, :], direct)
            padded = jnp.concatenate([direct, jnp.zeros((lanes - bands, lanes), F32)], axis=0)
            mirror = padded.T[:bands]
            if part:
                mirror = -mirror
            ref[part] = jnp.where(covered, direct, mirror)[:, :bands]


def general_matrices(psi, masked, applied, layout, scale):
    bands, count = layout.total, layout.count
    left = psi.reshape(2, count, -1)
    right = jnp.stack([masked.reshape(2, -1), applied.reshape(2, -1)])
    product = jnp.einsum("cin,mdn->mcdi", left, right, preferred_element_type=F32)
    block = jnp.stack([product[:, 0, 0] + product[:, 1, 1], product[:, 0, 1] - product[:, 1, 0]], axis=1)
    everywhere = lax.all_gather(lax.psum(block * scale, "ga"), "band", axis=0)
    slot = np.full((bands, bands), -1)
    for device in range(bands):
        for part in range(len(layout.parts)):
            for core in range(layout.nc):
                slot[device, layout.source(device, part, core)] = part * layout.nc + core
    flat = jnp.transpose(everywhere, (1, 2, 0, 3)).reshape(4 * bands, count)
    index = jnp.asarray(np.tile(np.maximum(slot, 0), (4, 1)), jnp.int32)
    direct = jnp.take_along_axis(flat, index, axis=1).reshape(2, 2, bands, bands)
    direct = jnp.swapaxes(direct, 2, 3)
    sign = jnp.asarray([1.0, -1.0], F32)[None, :, None, None]
    full = jnp.where(jnp.asarray(slot.T >= 0), direct, sign * jnp.swapaxes(direct, 2, 3))
    return full[0], full[1]


def body(band_total, groups, orbitals, potential, slot_sticks, stick_entries):
    _, points = potential.shape
    width = stick_entries.shape[1]
    radius = width // 2
    slots = orbitals.shape[2]
    layout = Bands(band_total)
    ga = lax.axis_index("ga").astype(jnp.int32).reshape(1)
    sticks = slot_sticks.reshape(1, groups * slots)
    tables = [jnp.asarray(t) for t in twiddle_tables(points, radius, groups)]

    rows = pl.pallas_call(
        rows_kernel,
        out_shape=jax.ShapeDtypeStruct((width, 128), F32),
        out_specs=VMEM_SPEC,
        compiler_params=KERNEL_PARAMS,
        cost_estimate=pl.CostEstimate(flops=FIRST_FLOPS, bytes_accessed=0, transcendentals=0),
        name="rows",
    )()
    sticks = pl.pallas_call(
        copy_kernel,
        out_shape=jax.ShapeDtypeStruct(sticks.shape, jnp.int32),
        in_specs=[VMEM_SPEC, VMEM_SPEC],
        out_specs=VMEM_SPEC,
        compiler_params=KERNEL_PARAMS,
        name="sticks",
    )(rows, sticks)
    others = []
    for distance in range(1, groups):
        pairs = [(i, (i + distance) % groups) for i in range(groups)]
        others.append(lax.ppermute(orbitals, "ga", pairs))
    near, far = [orbitals], []
    for part, way in enumerate(layout.parts):
        if way is None or (way[1] == 0 and part > 0):
            (far if way is None else near).append(lax.ppermute(orbitals, "band", layout.pairs(part)))

    chunks = pl.cdiv(groups * slots, 128)
    place = pl.pallas_call(
        place_kernel,
        out_shape=(
            jax.ShapeDtypeStruct((slots, 2 * width), BF16),
            jax.ShapeDtypeStruct((groups - 1, slots, width), jnp.int32),
            jax.ShapeDtypeStruct((groups, width, slots), BF16),
            jax.ShapeDtypeStruct((groups, slots, width), BF16),
            jax.ShapeDtypeStruct((slots, width), F32),
        ),
        in_specs=[SMEM_SPEC] + [VMEM_SPEC] * 4,
        out_specs=(VMEM_SPEC,) * 5,
        scratch_shapes=[pltpu.VMEM((chunks, width, 128), F32), pltpu.VMEM((chunks * 128, width), jnp.int32)],
        compiler_params=KERNEL_PARAMS,
        cost_estimate=pl.CostEstimate(flops=SPREAD_FLOPS, bytes_accessed=0, transcendentals=0),
        name="place",
    )
    coeffs, inverse, into, pick, kinetic = place(ga, rows, orbitals, stick_entries, sticks)
    coeffs, *near = lax.optimization_barrier((coeffs, *near))
    near = jnp.concatenate(near, axis=1)
    psi = [near]
    if layout.ny == 2:
        pairs = [(i, i ^ layout.nc) for i in range(band_total)]
        psi.append(lax.ppermute(near, "band", pairs))

    def run_grid(ga_ref, *refs):
        count = len(others)
        grid_kernel(ga_ref, refs[:count], *refs[count : count + 5], refs[count + 5 : count + 9], *refs[count + 9 :])

    grid = pl.pallas_call(
        run_grid,
        out_shape=(
            jax.ShapeDtypeStruct((slots, 2 * width), F32),
            jax.ShapeDtypeStruct((groups - 1, slots, 2 * width), F32),
        ),
        in_specs=[SMEM_SPEC] + [VMEM_SPEC] * (len(others) + 9),
        out_specs=(VMEM_SPEC, VMEM_SPEC),
        compiler_params=KERNEL_PARAMS,
        cost_estimate=pl.CostEstimate(flops=GRID_FLOPS, bytes_accessed=0, transcendentals=0),
        name="grid",
    )
    own, send = grid(ga, *others, coeffs, inverse, into, pick, potential, *tables)
    own, *far = lax.optimization_barrier((own, *far))
    psi = [jnp.concatenate(psi + far, axis=1)]
    if layout.nc == 2:
        psi.append(lax.ppermute(psi[0], "band", [(i, i ^ 1) for i in range(band_total)]))
    partials = [own]
    for distance in range(1, groups):
        pairs = [(i, (i + distance) % groups) for i in range(groups)]
        partials.append(lax.ppermute(send[distance - 1], "ga", pairs))

    scale = 1.0 / (4.0 * radius * radius)
    out_type = jax.ShapeDtypeStruct(orbitals.shape, BF16)
    small = 4 * layout.count <= 128 and band_total <= 128
    count = len(partials)
    if not small:

        def run_apply(ga_ref, *refs):
            result, _ = apply_part(ga_ref[0], refs[:count], *refs[count : count + 3], points)
            refs[count + 3][0, 0] = result[0]
            refs[count + 3][1, 0] = result[1]

        applied = pl.pallas_call(
            run_apply,
            out_shape=out_type,
            in_specs=[SMEM_SPEC] + [VMEM_SPEC] * (count + 3),
            out_specs=VMEM_SPEC,
            compiler_params=KERNEL_PARAMS,
            name="apply",
        )(ga, *partials, orbitals, stick_entries, kinetic)
        own_lists = lax.dynamic_slice_in_dim(stick_entries, ga[0] * slots, slots, 0)
        masked = jnp.where(own_lists >= 0, orbitals, jnp.zeros_like(orbitals))
        correlation, reduced = general_matrices(jnp.stack(psi, axis=2), masked, applied, layout, scale)
        return applied, correlation, reduced

    def run_final(ga_ref, *refs):
        psi_refs, outs = refs[count + 3 : count + 3 + len(psi)], refs[count + 3 + len(psi) :]
        final_kernel(points, ga_ref, refs[:count], *refs[count : count + 3], psi_refs, *outs)

    applied, sums = pl.pallas_call(
        run_final,
        out_shape=(out_type, jax.ShapeDtypeStruct((groups * band_total, 128), F32)),
        in_specs=[SMEM_SPEC] + [VMEM_SPEC] * (count + 3 + len(psi)),
        out_specs=(VMEM_SPEC, VMEM_SPEC),
        compiler_params=KERNEL_PARAMS,
        name="final",
    )(ga, *partials, orbitals, stick_entries, kinetic, *psi)
    everywhere = lax.all_to_all(sums, ("ga", "band"), split_axis=0, concat_axis=0, tiled=True)
    matrix = jax.ShapeDtypeStruct((2, band_total, band_total), F32)

    applied, correlation, reduced = pl.pallas_call(
        functools.partial(assemble_kernel, groups, layout, scale),
        out_shape=(out_type, matrix, matrix),
        in_specs=[VMEM_SPEC, VMEM_SPEC],
        out_specs=(VMEM_SPEC,) * 3,
        compiler_params=KERNEL_PARAMS,
        name="assemble",
    )(everywhere, applied)
    return applied, correlation, reduced


def solution(mesh):
    band_total = mesh.shape["band"]
    groups = mesh.shape["ga"]

    def mapped(orbitals, potential, slot_sticks, stick_entries):
        return body(band_total, groups, orbitals, potential, slot_sticks, stick_entries)

    return jax.shard_map(
        mapped,
        mesh=mesh,
        in_specs=(P(None, "band", "ga", None), P("ga", None), P(), P()),
        out_specs=(P(None, "band", "ga", None), P(), P()),
        check_vma=False,
    )
```

```python
import functools
import math

import jax
import jax.numpy as jnp
import numpy as np
from jax import lax
from jax.experimental import pallas as pl
from jax.experimental.pallas import tpu as pltpu
from jax.sharding import PartitionSpec as P


F32 = jnp.float32
BF16 = jnp.bfloat16
VMEM_SPEC = pl.BlockSpec(memory_space=pltpu.VMEM)
SMEM_SPEC = pl.BlockSpec(memory_space=pltpu.SMEM)
FIRST_FLOPS = 3_000_000_000
SPREAD_FLOPS = 1_500_000_000
GRID_FLOPS = 3_000_000_000
KERNEL_PARAMS = pltpu.CompilerParams(vmem_limit_bytes=16 * 1024 * 1024)


def hi_lo_table(values):
    high = jnp.asarray(values, F32).astype(BF16)
    high_np = np.asarray(values, np.float32).astype(jnp.bfloat16)
    low_np = (values - high_np.astype(np.float64)).astype(jnp.bfloat16)
    return high_np, low_np


def twiddle_tables(points, radius, group_count):
    width = 2 * radius
    planes = points // group_count
    z = np.arange(points, dtype=np.int64)
    gz = np.arange(width, dtype=np.int64) - radius + 1
    angle_z = (z[:, None] * gz[None, :] % points) * (2.0 * np.pi / points)
    forward = np.concatenate([np.cos(angle_z), np.sin(angle_z)], axis=1)
    forward = forward.reshape(group_count, planes, 2 * width)
    backward = np.ascontiguousarray(np.transpose(forward, (0, 2, 1)))
    gx = np.arange(radius, dtype=np.int64)
    angle_x = (gx[:, None] * z[None, :] % points) * (2.0 * np.pi / points)
    x_table = np.concatenate([np.cos(angle_x), np.sin(angle_x)], axis=0)
    z_high, z_low = hi_lo_table(forward)
    zt_high, zt_low = hi_lo_table(backward)
    x_high, x_low = hi_lo_table(x_table)
    xt = np.concatenate([x_high.T, x_low.T], axis=1)
    return np.concatenate([z_high, z_low], 1), np.stack([zt_high, zt_low], 1), np.stack([x_high, x_low]), xt


def split(values):
    high = values.astype(BF16)
    low = (values - high.astype(F32)).astype(BF16)
    return high, low


def dot(left, right):
    return jnp.dot(left, right, preferred_element_type=F32)


def dot_rows(left, right):
    return lax.dot_general(left, right, (((1,), (1,)), ((), ())), preferred_element_type=F32)


class Bands:
    def __init__(self, total):
        self.total = total
        self.inner = math.gcd(total, 4)
        self.blocks = total // self.inner
        self.ny = max(self.inner // 2, 1)
        self.nc = min(self.inner, 2)
        self.parts = [(s, y) for y in range(self.ny) for s in range((self.blocks + 1) // 2)]
        self.half = self.blocks // 2 if self.blocks % 2 == 0 else 0
        if self.half:
            self.parts.append(None)
        self.count = len(self.parts) * self.nc

    def source(self, device, part, other_core, where=np.where):
        block = device // self.inner if where is np.where else lax.div(device, self.inner)
        place = device - block * self.inner
        if self.parts[part] is None:
            turned = where(block < self.half, 0, self.ny - 1)
            block = where(block < self.half, block + self.half, block - self.half)
        else:
            shift, turned = self.parts[part]
            block = where(block < shift, block - shift + self.blocks, block - shift)
        return block * self.inner + (place ^ (turned * self.nc + other_core))

    def pairs(self, part):
        return [(int(self.source(device, part, 0)), device) for device in range(self.total)]


def canonical_lane(sticks, radius):
    gx = sticks - radius + 1
    return jnp.where(gx >= 0, gx, radius - gx)


def rows_kernel(out_ref):
    out_ref[...] = lax.broadcasted_iota(jnp.int32, out_ref.shape, 0).astype(F32)


def copy_kernel(_, in_ref, out_ref):
    out_ref[...] = in_ref[...]


def sticks_of(sticks_ref, group, slots):
    sticks = sticks_ref[...]
    row = sticks[:, :slots]
    for index in range(1, sticks.shape[1] // slots):
        row = jnp.where(group == index, sticks[:, index * slots : (index + 1) * slots], row)
    return row


def spread(values, inverse):
    index = jnp.maximum(inverse, 0)
    parts = []
    for part in values:
        moved = jnp.take_along_axis(part.astype(F32), index, axis=1, mode="promise_in_bounds")
        parts.append(jnp.where(inverse >= 0, moved, 0.0))
    return jnp.concatenate(parts, axis=1).astype(BF16)


def choose_slots(sticks_ref, group, slots, width):
    lane = canonical_lane(sticks_of(sticks_ref, group, slots), width // 2)
    return (lax.broadcasted_iota(jnp.int32, (width, slots), 0) == lane).astype(F32).astype(BF16)


def group_before(ga, distance, groups):
    return lax.rem(ga + (groups - distance), groups)


def place_kernel(
    ga_ref, rows_ref, orbitals_ref, entries_ref, sticks_ref, out_ref, inverse_ref, in_ref, pick_ref, kinetic_ref, e_ref, all_ref
):
    width = entries_ref.shape[1]
    slots = orbitals_ref.shape[2]
    total = entries_ref.shape[0]
    groups = total // slots
    radius = width // 2
    ga = ga_ref[0]
    chunks, _, lanes = e_ref.shape
    lists_t = entries_ref[...].astype(F32)
    position = rows_ref[...]
    for chunk in range(chunks):
        first = chunk * lanes
        used = min(lanes, total - first)
        copies = 1
        while used * copies * 2 <= lanes and lanes % (used * copies * 2) == 0:
            copies *= 2
        if used * copies < lanes:
            copies, used_rows = 1, jnp.concatenate([lists_t[first:], jnp.full((lanes - used, width), -1.0, F32)], axis=0)
        else:
            used_rows = jnp.concatenate([lists_t[first : first + used]] * copies, axis=0)
        e_ref[chunk] = used_rows.T
        height = width // copies
        target = position[:height]
        if copies > 1:
            lane = lax.broadcasted_iota(jnp.int32, (height, lanes), 1).astype(F32)
            for copy in range(1, copies):
                target = jnp.where(lane >= copy * used, position[:height] + copy * height, target)

        def step(k, found):
            match = e_ref[chunk, pl.ds(k, 1), :] == target
            return jnp.where(match, k.astype(F32), found)

        found = lax.fori_loop(0, width, step, jnp.full((height, lanes), -1.0, F32), unroll=8)
        if copies > 1:
            found = jnp.concatenate([found[:, c * used : (c + 1) * used] for c in range(copies)], axis=0)
        found = found.T.astype(jnp.int32)
        all_ref[first : first + found.shape[0], :] = found

    def lists(group):
        return all_ref[pl.ds(pl.multiple_of(group * slots, 8), slots), :]

    out_ref[...] = spread([orbitals_ref[0, 0], orbitals_ref[1, 0]], lists(ga))
    for distance in range(1, groups):
        inverse_ref[distance - 1] = lists(group_before(ga, distance, groups))
    lane = lax.broadcasted_iota(jnp.int32, (slots, width), 1)
    for distance in range(groups):
        in_ref[distance] = choose_slots(sticks_ref, group_before(ga, distance, groups), slots, width)
        row = canonical_lane(sticks_of(sticks_ref, lax.rem(ga + distance, groups), slots), radius).astype(F32)
        column = jnp.broadcast_to(row, (width, slots)).T.astype(jnp.int32)
        pick_ref[distance] = (column == lane).astype(F32).astype(BF16)
    gx_row = (sticks_of(sticks_ref, ga, slots) - radius + 1).astype(F32)
    gx = jnp.broadcast_to(gx_row, (width, slots)).T
    gz = (entries_ref[pl.ds(pl.multiple_of(ga * slots, 8), slots), :] - radius + 1).astype(F32)
    kinetic_ref[...] = (gx * gx + gz * gz) * (1.0 / (radius * radius))


def grid_kernel(ga_ref, other_refs, own_coeffs_ref, inverse_ref, in_ref, pick_ref, potential_ref, tables, own_ref, send_ref):
    z_table, zt_table, x_table, xt = tables
    planes, _ = potential_ref.shape
    width = own_coeffs_ref.shape[1] // 2
    radius = width // 2
    ga = ga_ref[0]
    coeffs = dot(in_ref[0], own_coeffs_ref[...])
    for distance, ref in enumerate(other_refs, 1):
        coeffs = coeffs + dot(in_ref[distance], spread([ref[0, 0], ref[1, 0]], inverse_ref[distance - 1]))
    real_part, imag_part = coeffs[:, :width], coeffs[:, width:]
    rows = jnp.concatenate(
        [
            jnp.concatenate([real_part, -imag_part], axis=1),
            jnp.concatenate([imag_part, real_part], axis=1),
        ],
        axis=0,
    ).astype(BF16)
    columns = dot_rows(z_table[ga], rows)
    columns = columns[:planes] + columns[planes:]
    col_re, col_im = columns[:, :width], columns[:, width:]
    rol_re, rol_im = pltpu.roll(col_re, radius, 1), pltpu.roll(col_im, radius, 1)
    even = lax.broadcasted_iota(jnp.int32, (planes, width), 1) < radius
    parity = jnp.concatenate(
        [
            jnp.where(even, col_re + rol_re, col_im - rol_im),
            jnp.where(even, col_im + rol_im, rol_re - col_re),
        ],
        axis=0,
    )
    par_high, par_low = split(parity)
    table = x_table[0]
    field = dot(jnp.concatenate([par_high, par_low], axis=1), jnp.concatenate([table, table], axis=0))
    field = field + dot(par_high, x_table[1])
    values = potential_ref[...]
    product = jnp.concatenate([values, values], axis=0) * field
    prod_high, prod_low = split(product)
    table_t = xt[...]
    wide = dot(prod_high, table_t)
    back = wide[:, :width] + wide[:, width:] + dot(prod_low, table_t[:, :width])
    back_re, back_im = back[:planes], back[planes:]
    rol_re, rol_im = pltpu.roll(back_re, radius, 1), pltpu.roll(back_im, radius, 1)
    gathered = jnp.concatenate(
        [
            jnp.where(even, back_re + rol_im, rol_re - back_im),
            jnp.where(even, back_im - rol_re, rol_im + back_re),
        ],
        axis=1,
    )
    gat_high, gat_low = split(gathered)
    spectra = dot(zt_table[ga, 0], gat_high) + dot(zt_table[ga, 1], gat_high) + dot(zt_table[ga, 0], gat_low)
    spectra = jnp.concatenate(
        [
            spectra[:width, :width] + spectra[width:, width:],
            spectra[:width, width:] - spectra[width:, :width],
        ],
        axis=0,
    )
    spec_high, spec_low = split(spectra)
    spec = jnp.concatenate([spec_high, spec_low], axis=1)
    for distance in range(pick_ref.shape[0]):
        choose = pick_ref[distance]
        picked = dot_rows(jnp.concatenate([choose, choose], axis=1), spec)
        if distance == 0:
            own_ref[...] = picked
        else:
            send_ref[distance - 1] = picked


def apply_part(ga, partial_refs, orbitals_ref, entries_ref, kinetic_ref, points):
    width = entries_ref.shape[1]
    slots = orbitals_ref.shape[2]
    total = partial_refs[0][...]
    for ref in partial_refs[1:]:
        total = total + ref[...]
    entries = entries_ref[pl.ds(pl.multiple_of(ga * slots, 8), slots), :]
    present = entries >= 0
    index = jnp.maximum(entries, 0)
    kinetic = kinetic_ref[...]
    result = []
    for part in range(2):
        picked = jnp.take_along_axis(
            total[:, part * width : (part + 1) * width], index, axis=1, mode="promise_in_bounds"
        )
        value = kinetic * orbitals_ref[part, 0].astype(F32) + picked * (1.0 / (points * points))
        result.append(jnp.where(present, value, 0.0).astype(BF16))
    return result, present


def final_kernel(points, ga_ref, partial_refs, orbitals_ref, entries_ref, kinetic_ref, psi_refs, out_ref, sums_ref):
    ga = ga_ref[0]
    result, present = apply_part(ga, partial_refs, orbitals_ref, entries_ref, kinetic_ref, points)
    for part in range(2):
        out_ref[part, 0] = result[part]
    _, width = present.shape
    h_re, h_im = result[0].astype(F32), result[1].astype(F32)
    m_re = jnp.where(present, orbitals_ref[0, 0].astype(F32), 0.0)
    m_im = jnp.where(present, orbitals_ref[1, 0].astype(F32), 0.0)
    rows = [[], [], [], []]
    for part in range(psi_refs[0].shape[1]):
        for psi_ref in psi_refs:
            left_re = psi_ref[0, part].astype(F32)
            left_im = psi_ref[1, part].astype(F32)
            for place, (right_re, right_im) in enumerate(((m_re, m_im), (h_re, h_im))):
                rows[2 * place].append(jnp.sum(left_re * right_re + left_im * right_im, axis=0, keepdims=True))
                rows[2 * place + 1].append(jnp.sum(left_re * right_im - left_im * right_re, axis=0, keepdims=True))
    flat = sum(rows, [])
    lanes = sums_ref.shape[1]
    if len(flat) < lanes:
        flat.append(jnp.zeros((lanes - len(flat), width), F32))
    sums = jnp.sum(jnp.concatenate(flat, axis=0).T, axis=0, keepdims=True)
    sums_ref[...] = jnp.broadcast_to(sums, sums_ref.shape)


def assemble_kernel(groups, layout, scale, sums_ref, applied_ref, out_ref, corr_ref, ham_ref):
    out_ref[...] = applied_ref[...]
    bands = layout.total
    total = sums_ref[0:bands, :]
    for group in range(1, groups):
        total = total + sums_ref[group * bands : (group + 1) * bands, :]
    lanes = total.shape[1]
    total = jnp.concatenate([total, jnp.zeros((lanes - bands, lanes), F32)], axis=0).T * scale
    row = lax.broadcasted_iota(jnp.int32, (bands, lanes), 0)
    col = lax.broadcasted_iota(jnp.int32, (bands, lanes), 1)
    matches = []
    for part in range(len(layout.parts)):
        for core in range(layout.nc):
            matches.append(row == layout.source(col, part, core, jnp.where))
    covered = functools.reduce(jnp.logical_or, matches)
    for place, ref in enumerate((corr_ref, ham_ref)):
        for part in range(2):
            base = (2 * place + part) * layout.count
            direct = jnp.zeros((bands, lanes), F32)
            for index, match in enumerate(matches):
                direct = jnp.where(match, total[base + index : base + index + 1, :], direct)
            padded = jnp.concatenate([direct, jnp.zeros((lanes - bands, lanes), F32)], axis=0)
            mirror = padded.T[:bands]
            if part:
                mirror = -mirror
            ref[part] = jnp.where(covered, direct, mirror)[:, :bands]


def general_matrices(psi, masked, applied, layout, scale):
    bands, count = layout.total, layout.count
    left = psi.reshape(2, count, -1)
    right = jnp.stack([masked.reshape(2, -1), applied.reshape(2, -1)])
    product = jnp.einsum("cin,mdn->mcdi", left, right, preferred_element_type=F32)
    block = jnp.stack([product[:, 0, 0] + product[:, 1, 1], product[:, 0, 1] - product[:, 1, 0]], axis=1)
    everywhere = lax.all_gather(lax.psum(block * scale, "ga"), "band", axis=0)
    slot = np.full((bands, bands), -1)
    for device in range(bands):
        for part in range(len(layout.parts)):
            for core in range(layout.nc):
                slot[device, layout.source(device, part, core)] = part * layout.nc + core
    flat = jnp.transpose(everywhere, (1, 2, 0, 3)).reshape(4 * bands, count)
    index = jnp.asarray(np.tile(np.maximum(slot, 0), (4, 1)), jnp.int32)
    direct = jnp.take_along_axis(flat, index, axis=1).reshape(2, 2, bands, bands)
    direct = jnp.swapaxes(direct, 2, 3)
    sign = jnp.asarray([1.0, -1.0], F32)[None, :, None, None]
    full = jnp.where(jnp.asarray(slot.T >= 0), direct, sign * jnp.swapaxes(direct, 2, 3))
    return full[0], full[1]


def body(band_total, groups, orbitals, potential, slot_sticks, stick_entries):
    _, points = potential.shape
    width = stick_entries.shape[1]
    radius = width // 2
    slots = orbitals.shape[2]
    layout = Bands(band_total)
    ga = lax.axis_index("ga").astype(jnp.int32).reshape(1)
    sticks = slot_sticks.reshape(1, groups * slots)
    tables = [jnp.asarray(t) for t in twiddle_tables(points, radius, groups)]

    set_rows = pl.pallas_call(
        rows_kernel,
        out_shape=jax.ShapeDtypeStruct((width, 128), F32),
        out_specs=VMEM_SPEC,
        compiler_params=KERNEL_PARAMS,
        cost_estimate=pl.CostEstimate(flops=FIRST_FLOPS, bytes_accessed=0, transcendentals=0),
        name="rows",
    )
    copy_sticks = pl.pallas_call(
        copy_kernel,
        out_shape=jax.ShapeDtypeStruct(sticks.shape, jnp.int32),
        in_specs=[VMEM_SPEC, VMEM_SPEC],
        out_specs=VMEM_SPEC,
        compiler_params=KERNEL_PARAMS,
        name="sticks",
    )
    rows = set_rows()
    sticks = copy_sticks(rows, sticks)
    others = []
    for distance in range(1, groups):
        pairs = [(i, (i + distance) % groups) for i in range(groups)]
        others.append(lax.ppermute(orbitals, "ga", pairs))
    near, far = [orbitals], []
    for part, way in enumerate(layout.parts):
        if way is None or (way[1] == 0 and part > 0):
            (far if way is None else near).append(lax.ppermute(orbitals, "band", layout.pairs(part)))

    chunks = pl.cdiv(groups * slots, 128)
    place = pl.pallas_call(
        place_kernel,
        out_shape=(
            jax.ShapeDtypeStruct((slots, 2 * width), BF16),
            jax.ShapeDtypeStruct((groups - 1, slots, width), jnp.int32),
            jax.ShapeDtypeStruct((groups, width, slots), BF16),
            jax.ShapeDtypeStruct((groups, slots, width), BF16),
            jax.ShapeDtypeStruct((slots, width), F32),
        ),
        in_specs=[SMEM_SPEC] + [VMEM_SPEC] * 4,
        out_specs=(VMEM_SPEC,) * 5,
        scratch_shapes=[pltpu.VMEM((chunks, width, 128), F32), pltpu.VMEM((chunks * 128, width), jnp.int32)],
        compiler_params=KERNEL_PARAMS,
        cost_estimate=pl.CostEstimate(flops=SPREAD_FLOPS, bytes_accessed=0, transcendentals=0),
        name="place",
    )
    coeffs, inverse, into, pick, kinetic = place(ga, rows, orbitals, stick_entries, sticks)
    coeffs, *near = lax.optimization_barrier((coeffs, *near))
    near = jnp.concatenate(near, axis=1)
    psi = [near]
    if layout.ny == 2:
        pairs = [(i, i ^ layout.nc) for i in range(band_total)]
        psi.append(lax.ppermute(near, "band", pairs))

    def run_grid(ga_ref, *refs):
        count = len(others)
        grid_kernel(ga_ref, refs[:count], *refs[count : count + 5], refs[count + 5 : count + 9], *refs[count + 9 :])

    grid = pl.pallas_call(
        run_grid,
        out_shape=(
            jax.ShapeDtypeStruct((slots, 2 * width), F32),
            jax.ShapeDtypeStruct((groups - 1, slots, 2 * width), F32),
        ),
        in_specs=[SMEM_SPEC] + [VMEM_SPEC] * (len(others) + 9),
        out_specs=(VMEM_SPEC, VMEM_SPEC),
        compiler_params=KERNEL_PARAMS,
        cost_estimate=pl.CostEstimate(flops=GRID_FLOPS, bytes_accessed=0, transcendentals=0),
        name="grid",
    )
    own, send = grid(ga, *others, coeffs, inverse, into, pick, potential, *tables)
    own, *far = lax.optimization_barrier((own, *far))
    psi = [jnp.concatenate(psi + far, axis=1)]
    if layout.nc == 2:
        psi.append(lax.ppermute(psi[0], "band", [(i, i ^ 1) for i in range(band_total)]))
    partials = [own]
    for distance in range(1, groups):
        pairs = [(i, (i + distance) % groups) for i in range(groups)]
        partials.append(lax.ppermute(send[distance - 1], "ga", pairs))

    scale = 1.0 / (4.0 * radius * radius)
    out_type = jax.ShapeDtypeStruct(orbitals.shape, BF16)
    small = 4 * layout.count <= 128 and band_total <= 128
    count = len(partials)
    if not small:

        def run_apply(ga_ref, *refs):
            result, _ = apply_part(ga_ref[0], refs[:count], *refs[count : count + 3], points)
            refs[count + 3][0, 0] = result[0]
            refs[count + 3][1, 0] = result[1]

        applied = pl.pallas_call(
            run_apply,
            out_shape=out_type,
            in_specs=[SMEM_SPEC] + [VMEM_SPEC] * (count + 3),
            out_specs=VMEM_SPEC,
            compiler_params=KERNEL_PARAMS,
            name="apply",
        )(ga, *partials, orbitals, stick_entries, kinetic)
        own_lists = lax.dynamic_slice_in_dim(stick_entries, ga[0] * slots, slots, 0)
        masked = jnp.where(own_lists >= 0, orbitals, jnp.zeros_like(orbitals))
        correlation, reduced = general_matrices(jnp.stack(psi, axis=2), masked, applied, layout, scale)
        return applied, correlation, reduced

    def run_final(ga_ref, *refs):
        psi_refs, outs = refs[count + 3 : count + 3 + len(psi)], refs[count + 3 + len(psi) :]
        final_kernel(points, ga_ref, refs[:count], *refs[count : count + 3], psi_refs, *outs)

    applied, sums = pl.pallas_call(
        run_final,
        out_shape=(out_type, jax.ShapeDtypeStruct((groups * band_total, 128), F32)),
        in_specs=[SMEM_SPEC] + [VMEM_SPEC] * (count + 3 + len(psi)),
        out_specs=(VMEM_SPEC, VMEM_SPEC),
        compiler_params=KERNEL_PARAMS,
        name="final",
    )(ga, *partials, orbitals, stick_entries, kinetic, *psi)
    everywhere = lax.all_to_all(sums, ("ga", "band"), split_axis=0, concat_axis=0, tiled=True)
    matrix = jax.ShapeDtypeStruct((2, band_total, band_total), F32)

    applied, correlation, reduced = pl.pallas_call(
        functools.partial(assemble_kernel, groups, layout, scale),
        out_shape=(out_type, matrix, matrix),
        in_specs=[VMEM_SPEC, VMEM_SPEC],
        out_specs=(VMEM_SPEC,) * 3,
        compiler_params=KERNEL_PARAMS,
        name="assemble",
    )(everywhere, applied)
    return applied, correlation, reduced


def solution(mesh):
    band_total = mesh.shape["band"]
    groups = mesh.shape["ga"]

    def mapped(orbitals, potential, slot_sticks, stick_entries):
        return body(band_total, groups, orbitals, potential, slot_sticks, stick_entries)

    return jax.shard_map(
        mapped,
        mesh=mesh,
        in_specs=(P(None, "band", "ga", None), P("ga", None), P(), P()),
        out_specs=(P(None, "band", "ga", None), P(), P()),
        check_vma=False,
    )
```
